32 devices in a mesh: rep: 8 (over z, core), tp: 4 (over y, x).
Axes of the slice: x: 2, y: 2, z: 4, core: 2. Of those that a mesh axis runs over, the one named last changes fastest.
Arguments:
- queries: bfloat16 [64, 8192], P('rep', 'tp'), may hold values from -200 to 200
- new_keys: bfloat16 [64, 1024], P('rep', 'tp'), may hold values from -6 to 6
- new_values: bfloat16 [64, 1024], P('rep', 'tp'), may hold values from -6 to 6
- key_pool: bfloat16 [768, 128, 1024], P('rep', 'tp'), may hold values from -6 to 6
- value_pool: bfloat16 [768, 128, 1024], P('rep', 'tp'), may hold values from -6 to 6
- lengths: int32 [64], replicated, may hold values from 1 to 1536, as said below
- page_table: int32 [64, 12], P('rep'), may hold values from -1 to 95, as said below
- mig_slot: int32 [8], replicated, may hold values from 0 to 7
- mig_dst: int32 [8], replicated, may hold values from 0 to 7, as said below
Outputs:
- attended: bfloat16 [64, 8192], P('rep', 'tp')
- moved_keys: bfloat16 [96, 128, 1024], P('rep', 'tp')
- moved_values: bfloat16 [96, 128, 1024], P('rep', 'tp')
The draws below stay inside these ranges and needn't reach their ends.
Inputs may be any that keep to these rules, and one draw needn't show every extreme that they name: mig_dst[r] = (r + c) mod 8 for one offset c with 1 <= c < 8, the same for every replica. `page_table`: row q lists distinct pool pages of its replica for its first ceil(lengths[q] / 128) pages and -1 after them. `lengths`: some request has exactly 1536 cached tokens.
All inputs are finite; a program needn't handle non-finite values.
Results may differ from the reference program's by a relative error of at most 0.0065.
Values may be sent and summed in bfloat16 or wider, within the bound.
A program may use at most 64 MiB of HBM per device.

```python
import math
import jax
import jax.numpy as jnp
from jax import lax

H = 64
KVH = 8
DH = 128
PAGE = 128
PAGES_REQ = 12
REQ_REP = 8
REPLICAS = 8
REQS = 64
POOL = 96
N_REP = 8


def live_lengths(key):
    drawn = jax.random.randint(jax.random.fold_in(key, 101), (REQS,), 1, PAGES_REQ * PAGE + 1)
    return drawn.at[0].set(PAGES_REQ * PAGE).astype(jnp.int32)


def draw_lengths(key, part):
    return live_lengths(key)


def draw_page_table(key, part):
    cached = live_lengths(key)
    page_count = (cached + PAGE - 1) // PAGE
    replica_keys = jax.random.split(jax.random.fold_in(key, 202), REPLICAS)
    orders = jax.vmap(lambda subkey: jax.random.permutation(subkey, POOL))(replica_keys)
    tables = orders.reshape(REQS, PAGES_REQ).astype(jnp.int32)
    columns = jnp.arange(PAGES_REQ, dtype=jnp.int32)
    return jnp.where(columns[None, :] < page_count[:, None], tables, -1).astype(jnp.int32)


def draw_mig_dst(key, part):
    stride = jax.random.randint(jax.random.fold_in(key, 303), (), 1, REPLICAS)
    return ((jnp.arange(REPLICAS, dtype=jnp.int32) + stride) % REPLICAS).astype(jnp.int32)


def draw_queries(key, part):
    base = jnp.clip(jax.random.normal(key, (REQS, H * DH), jnp.float32), -5.0, 5.0)
    base = base * 1.5
    return base.astype(jnp.bfloat16)


def with_ends(result, key, least, top_value):
    extent = result.shape
    spot = [jax.random.randint(jax.random.fold_in(key, axis), (), 0, extent[axis]) for axis in range(len(extent))]
    result = result.at[tuple(spot)].set(least)
    longest = extent.index(max(extent))
    spot[longest] = (spot[longest] + 1) % extent[longest]
    return result.at[tuple(spot)].set(top_value)


def levels(key, shape, cuts, low, top_value):
    gain, own = 1.0, jax.random.fold_in(key, 6)
    for position, parts in cuts:
        draws = jnp.exp(jax.random.uniform(jax.random.fold_in(own, position), (parts,), jnp.float32, low / len(cuts), top_value / len(cuts)))
        gain = gain * jnp.repeat(draws, shape[position] // parts).reshape([-1 if axis == position else 1 for axis in range(len(shape))])
    return gain


def scatter_about(key, shape, spread, most, shards=(), kind=jnp.bfloat16):
    values = spread * jax.random.normal(key, shape, jnp.float32)
    if shards:
        values = values * levels(key, shape, shards, -0.22, 0.18)
    return jnp.clip(values, -most, most).astype(kind)


def setup_inputs(seed: int = 0) -> dict:
    keys = jax.random.split(jax.random.key(seed), 10)
    return {
        "queries": draw_queries(jax.random.fold_in(keys[9], 71), 0),
        "new_keys": scatter_about(keys[1], (REQS, KVH * DH), 1.5, 6.0, ((0, 8), (1, 4))),
        "new_values": scatter_about(keys[2], (REQS, KVH * DH), 1.0, 6.0, ((0, 8), (1, 4))),
        "key_pool": scatter_about(keys[3], (N_REP * POOL, PAGE, KVH * DH), 1.0, 6.0, ((0, 8), (1, 4))),
        "value_pool": scatter_about(keys[4], (N_REP * POOL, PAGE, KVH * DH), 1.0, 6.0, ((0, 8), (1, 4))),
        "lengths": draw_lengths(jax.random.fold_in(keys[9], 71), 0),
        "page_table": draw_page_table(jax.random.fold_in(keys[9], 71), 0),
        "mig_slot": with_ends(jax.random.randint(keys[7], (REPLICAS,), 0, REQ_REP), jax.random.fold_in(keys[7], 1), 0, REQ_REP - 1).astype(jnp.int32),
        "mig_dst": draw_mig_dst(jax.random.fold_in(keys[9], 71), 0),
    }


def reference(queries, new_keys, new_values, key_pool, value_pool, lengths, page_table, mig_slot, mig_dst):
    replica_ids = jnp.arange(N_REP, dtype=jnp.int32)
    scaling = 1.0 / math.sqrt(DH)

    def one_replica(replica):
        source = jnp.sum(jnp.where(mig_dst == replica, replica_ids, 0)).astype(jnp.int32)
        leaving = mig_slot[replica]
        arriving = (source * REQ_REP + mig_slot[source]).astype(jnp.int32)
        slot_ids = jnp.arange(REQ_REP, dtype=jnp.int32)
        owner_rep = jnp.where(slot_ids == leaving, source, replica).astype(jnp.int32)
        owner_req = jnp.where(slot_ids == leaving, arriving, replica * REQ_REP + slot_ids).astype(jnp.int32)
        table_rows = page_table[owner_req]
        page_index = (owner_rep[:, None] * POOL + jnp.maximum(table_rows, 0)).astype(jnp.int32)
        cached_keys = key_pool[page_index].reshape(REQ_REP, PAGES_REQ * PAGE, KVH, DH).astype(jnp.float32)
        cached_values = value_pool[page_index].reshape(REQ_REP, PAGES_REQ * PAGE, KVH, DH).astype(jnp.float32)
        live_len = lengths[owner_req]
        positions = jnp.arange(PAGES_REQ * PAGE, dtype=jnp.int32)
        usable = positions[None, :] < live_len[:, None]
        start = (replica * REQ_REP).astype(jnp.int32)
        query_rows = lax.dynamic_slice_in_dim(queries, start, REQ_REP, 0).reshape(REQ_REP, KVH, H // KVH, DH).astype(jnp.float32)
        fresh_keys = lax.dynamic_slice_in_dim(new_keys, start, REQ_REP, 0).reshape(REQ_REP, KVH, DH).astype(jnp.float32)
        fresh_values = lax.dynamic_slice_in_dim(new_values, start, REQ_REP, 0).reshape(REQ_REP, KVH, DH).astype(jnp.float32)
        scores = jnp.einsum('rgqd,rngd->rgqn', query_rows, cached_keys) * scaling
        new_score = jnp.einsum('rgqd,rgd->rgq', query_rows, fresh_keys) * scaling
        masked = jnp.where(usable[:, None, None, :], scores, -jnp.inf)
        maxima = jnp.maximum(masked.max(-1), new_score)
        weights = jnp.where(usable[:, None, None, :], jnp.exp(masked - maxima[..., None]), 0.0)
        new_weight = jnp.exp(new_score - maxima)
        totals = weights.sum(-1) + new_weight
        rounded = lax.optimization_barrier(weights.astype(jnp.bfloat16)).astype(jnp.float32)
        rounded_new = lax.optimization_barrier(new_weight.astype(jnp.bfloat16)).astype(jnp.float32)
        mixed = jnp.einsum('rgqn,rngd->rgqd', rounded, cached_values)
        mixed = mixed + rounded_new[..., None] * fresh_values[:, :, None, :]
        attended = (mixed / totals[..., None]).reshape(REQ_REP, H * DH).astype(jnp.bfloat16)
        moved_rows = page_table[arriving]
        moved_index = (source * POOL + jnp.maximum(moved_rows, 0)).astype(jnp.int32)
        present = (moved_rows >= 0)[:, None, None]
        moved_keys = jnp.where(present, key_pool[moved_index], jnp.zeros((), jnp.bfloat16))
        moved_values = jnp.where(present, value_pool[moved_index], jnp.zeros((), jnp.bfloat16))
        return (attended, moved_keys, moved_values)
    attended, moved_keys, moved_values = lax.map(one_replica, replica_ids)
    return (attended.reshape(N_REP * REQ_REP, H * DH), moved_keys.reshape(N_REP * PAGES_REQ, PAGE, KVH * DH), moved_values.reshape(N_REP * PAGES_REQ, PAGE, KVH * DH))
```

```python
import functools
import math


import jax
import jax.numpy as jnp
from jax import lax
from jax.experimental import pallas as pl
from jax.experimental.pallas import tpu as pltpu
from jax.sharding import PartitionSpec as P

H = 64
KVH = 8
DH = 128
LOW = -1e30


def route_by(count, distance):
    return [(i, (i + distance) % count) for i in range(count)]


def pick_kernel(
    table_ref, mig_ref, q_ref, nk_ref, nv_ref, key_ref, value_ref, row_ref, kout_ref, vout_ref, sems
):
    pages = kout_ref.shape[0]
    leaving = mig_ref[lax.axis_index("rep")]

    @pl.loop(0, pages)
    def _(j):
        page = jnp.maximum(table_ref[leaving, j], 0)
        pltpu.make_async_copy(key_ref.at[page], kout_ref.at[j], sems.at[0]).start()
        pltpu.make_async_copy(value_ref.at[page], vout_ref.at[j], sems.at[1]).start()

    at = 0
    for ref in (q_ref, nk_ref, nv_ref):
        width = ref.shape[1]
        slot = lax.broadcasted_iota(jnp.int32, ref.shape, 0)
        chosen = jnp.where(slot == leaving, ref[...].astype(jnp.float32), 0.0)
        row = jnp.sum(chosen, axis=0, keepdims=True)
        row_ref[:, at : at + width] = row.astype(jnp.bfloat16)
        at += width
    pltpu.make_async_copy(key_ref.at[pl.ds(0, pages)], kout_ref, sems.at[0]).wait()
    pltpu.make_async_copy(value_ref.at[pl.ds(0, pages)], vout_ref, sems.at[1]).wait()

    @pl.loop(0, pages)
    def _(j):
        @pl.when(table_ref[leaving, j] < 0)
        def _():
            kout_ref[j] = jnp.zeros(kout_ref.shape[1:], kout_ref.dtype)
            vout_ref[j] = jnp.zeros(vout_ref.shape[1:], vout_ref.dtype)


def picked(table, mig_slot, queries, new_keys, new_values, key_pool, value_pool):
    shape = (table.shape[1],) + key_pool.shape[1:]
    width = queries.shape[1] + 2 * new_keys.shape[1]
    return pl.pallas_call(
        pick_kernel,
        out_shape=[
            jax.ShapeDtypeStruct((1, width), jnp.bfloat16),
            jax.ShapeDtypeStruct(shape, key_pool.dtype),
            jax.ShapeDtypeStruct(shape, key_pool.dtype),
        ],
        in_specs=[pl.BlockSpec(memory_space=pltpu.SMEM)] * 2
        + [pl.BlockSpec(memory_space=pltpu.VMEM)] * 3
        + [pl.BlockSpec(memory_space=pl.ANY)] * 2,
        out_specs=[pl.BlockSpec(memory_space=pltpu.VMEM)] * 3,
        scratch_shapes=[pltpu.SemaphoreType.DMA((2,))],
        compiler_params=pltpu.CompilerParams(vmem_limit_bytes=8 << 20),
        cost_estimate=pl.CostEstimate(
            flops=0, bytes_accessed=8 * math.prod(shape), transcendentals=0
        ),
    )(table, mig_slot, queries, new_keys, new_values, key_pool, value_pool)


def greet(parts):
    me = lax.axis_index("tp")
    barrier = pltpu.get_barrier_semaphore()
    for k in range(1, parts):
        pl.semaphore_signal(
            barrier,
            inc=1,
            device_id={"tp": lax.rem(me + k, parts)},
            device_id_type=pl.DeviceIdType.MESH,
        )
    pl.semaphore_wait(barrier, parts - 1)
    return me


def share_kernel(mig_ref, back_ref, tokens_ref, all_ref, mine_ref, own, send_sems, recv_sems):
    parts, slots, heads_here, _ = all_ref.shape
    chunks = tokens_ref.shape[1]
    leaving = mig_ref[lax.axis_index("rep")]
    back = back_ref[...].astype(jnp.float32)
    row = jnp.concatenate([back[:, h * DH : (h + 1) * DH] for h in range(chunks)], axis=0)
    for i in range(slots):
        value = jnp.where(leaving == i, row, tokens_ref[i].astype(jnp.float32))
        value = value.astype(jnp.bfloat16)
        mine_ref[i] = value
        own[i] = value[:heads_here]
    me = greet(parts)
    copies = []
    for k in range(1, parts):
        copy = pltpu.make_async_remote_copy(
            src_ref=own,
            dst_ref=all_ref.at[me],
            send_sem=send_sems.at[k - 1],
            recv_sem=recv_sems.at[k - 1],
            device_id={"tp": lax.rem(me + k, parts)},
            device_id_type=pl.DeviceIdType.MESH,
        )
        copy.start()
        copies.append(copy)
    all_ref[me] = own[...]
    for copy in copies:
        copy.wait()


def shared(mig_slot, back, tokens, heads_here, parts):
    slots = tokens.shape[0]
    return pl.pallas_call(
        share_kernel,
        out_shape=[
            jax.ShapeDtypeStruct((parts, slots, heads_here, DH), jnp.bfloat16),
            jax.ShapeDtypeStruct(tokens.shape, jnp.bfloat16),
        ],
        in_specs=[pl.BlockSpec(memory_space=pltpu.SMEM)]
        + [pl.BlockSpec(memory_space=pltpu.VMEM)] * 2,
        out_specs=[pl.BlockSpec(memory_space=pltpu.VMEM)] * 2,
        scratch_shapes=[
            pltpu.VMEM((slots, heads_here, DH), jnp.bfloat16),
            pltpu.SemaphoreType.DMA((parts - 1,)),
            pltpu.SemaphoreType.DMA((parts - 1,)),
        ],
        compiler_params=pltpu.CompilerParams(
            collective_id=0, has_side_effects=True, vmem_limit_bytes=8 << 20
        ),
        cost_estimate=pl.CostEstimate(flops=0, bytes_accessed=8 << 20, transcendentals=0),
    )(mig_slot, back, tokens)


def flat_rows(block):
    pages, rows, width = block.shape
    if rows % 16 == 0:
        return block.reshape(pages * rows, width)
    return block.astype(jnp.float32).reshape(pages * rows, width).astype(block.dtype)


def attend_kernel(
    table_ref,
    len_ref,
    start_ref,
    q_ref,
    key_ref,
    value_ref,
    out_ref,
    kbuf,
    vbuf,
    stats_ref,
    ksem,
    vsem,
):
    slots, pages, rows, width = kbuf.shape
    parts, heads_here = q_ref.shape[0], q_ref.shape[2]
    group = H // KVH
    page_len = rows * parts
    scaling = 1.0 / math.sqrt(DH)
    steps = 3 if pages % 3 == 0 else 1
    step_pages = pages // steps

    def live_pages(i):
        return lax.div(len_ref[i] + (page_len - 1), page_len)

    def key_copy(i, j):
        page = jnp.maximum(table_ref[i, j], 0)
        return pltpu.make_async_copy(key_ref.at[page], kbuf.at[i, j], ksem.at[i, j])

    def value_copy(i, j):
        page = jnp.maximum(table_ref[i, j], 0)
        return pltpu.make_async_copy(value_ref.at[page], vbuf.at[i, j], vsem.at[i, j])

    @pl.loop(0, slots)
    def _(i):
        @pl.loop(0, live_pages(i))
        def _(j):
            key_copy(i, j).start()
            value_copy(i, j).start()

    head = lax.broadcasted_iota(jnp.int32, (H, DH), 0) // group
    column = lax.broadcasted_iota(jnp.int32, (H, DH), 1)
    stats_ref[...] = jnp.zeros_like(stats_ref)

    def attend(i, used):
        tokens = used * rows
        lane = lax.broadcasted_iota(jnp.int32, (H, tokens), 1)
        position = (lane // rows) * page_len + lane % rows + start_ref[0]
        q = jnp.concatenate([q_ref[t, i].astype(jnp.float32) for t in range(parts)], axis=0)
        spread = jnp.concatenate(
            [jnp.where(head == g, q, 0.0).astype(jnp.bfloat16) for g in range(KVH)], axis=1
        )
        scores = lax.dot_general(
            spread,
            flat_rows(kbuf[i, 0:used]),
            (((1,), (1,)), ((), ())),
            preferred_element_type=jnp.float32,
        )
        usable = position < len_ref[i]
        masked = jnp.where(usable, scores * scaling, LOW)
        peak = jnp.max(masked, axis=1, keepdims=True)
        weights = jnp.where(usable, jnp.exp(masked - peak), 0.0)
        total = jnp.sum(weights, axis=1, keepdims=True)
        mixed = jnp.dot(
            weights.astype(jnp.bfloat16),
            flat_rows(vbuf[i, 0:used]),
            preferred_element_type=jnp.float32,
        )
        own = jnp.concatenate(
            [
                mixed[g * group : (g + 1) * group, g * DH : (g + 1) * DH]
                for g in range(KVH)
            ],
            axis=0,
        )
        for t in range(parts):
            out_ref[t, i] = own[t * heads_here : (t + 1) * heads_here]
        stats = jnp.where(column == i, peak, stats_ref[...])
        stats_ref[...] = jnp.where(column == i + slots, total, stats)

    @pl.loop(0, slots)
    def _(i):
        live = live_pages(i)
        needed = lax.div(live + (step_pages - 1), step_pages)

        @pl.loop(live, needed * step_pages)
        def _(j):
            vbuf[i, j] = jnp.zeros((rows, width), vbuf.dtype)

        @pl.loop(0, live)
        def _(j):
            key_copy(i, j).wait()
            value_copy(i, j).wait()

        for step in range(1, steps + 1):

            @pl.when(needed == step)
            def _():
                attend(i, step * step_pages)

    for t in range(parts):
        out_ref[t, slots] = stats_ref[t * heads_here : (t + 1) * heads_here]


def attended_parts(table, lens, start, q, key_pool, value_pool, parts):
    slots, pages = table.shape
    rows, width = key_pool.shape[1:]
    buffer = (slots, pages, rows, width)
    return pl.pallas_call(
        attend_kernel,
        out_shape=jax.ShapeDtypeStruct((parts, slots + 1, H // parts, DH), jnp.float32),
        in_specs=[pl.BlockSpec(memory_space=pltpu.SMEM)] * 3
        + [pl.BlockSpec(memory_space=pltpu.VMEM)]
        + [pl.BlockSpec(memory_space=pl.ANY)] * 2,
        out_specs=pl.BlockSpec(memory_space=pltpu.VMEM),
        scratch_shapes=[
            pltpu.VMEM(buffer, key_pool.dtype),
            pltpu.VMEM(buffer, value_pool.dtype),
            pltpu.VMEM((H, DH), jnp.float32),
            pltpu.SemaphoreType.DMA((slots, pages)),
            pltpu.SemaphoreType.DMA((slots, pages)),
        ],
        compiler_params=pltpu.CompilerParams(vmem_limit_bytes=24 << 20),
        cost_estimate=pl.CostEstimate(
            flops=4 * H * pages * rows * width * slots,
            bytes_accessed=4 * math.prod(buffer),
            transcendentals=0,
        ),
    )(table, lens, start, q, key_pool, value_pool)


def finish_kernel(
    mig_ref,
    part_ref,
    mine_ref,
    tk_ref,
    tv_ref,
    out_ref,
    leaver_ref,
    flat,
    landed,
    send_sems,
    recv_sems,
):
    parts, _, heads_here, _ = part_ref.shape
    slots = mine_ref.shape[0]
    repeat = heads_here // tk_ref.shape[1]
    leaving = mig_ref[lax.axis_index("rep")]
    scaling = 1.0 / math.sqrt(DH)
    me = greet(parts)
    copies = []
    for k in range(1, parts):
        peer = lax.rem(me + k, parts)
        copy = pltpu.make_async_remote_copy(
            src_ref=part_ref.at[peer],
            dst_ref=landed.at[k - 1],
            send_sem=send_sems.at[k - 1],
            recv_sem=recv_sems.at[k - 1],
            device_id={"tp": peer},
            device_id_type=pl.DeviceIdType.MESH,
        )
        copy.start()
        copies.append(copy)

    def spread(ref, i):
        value = ref[i].astype(jnp.float32)
        return jnp.concatenate(
            [
                jnp.broadcast_to(value[g : g + 1], (repeat, DH))
                for g in range(value.shape[0])
            ],
            axis=0,
        )

    fresh, values = [], []
    for i in range(slots):
        q = mine_ref[i].astype(jnp.float32)[:heads_here]
        fresh.append(jnp.sum(q * spread(tk_ref, i), axis=-1, keepdims=True) * scaling)
        values.append(spread(tv_ref, i))
    for copy in copies:
        copy.wait()
    stats = [part_ref[me, slots]] + [landed[k, slots] for k in range(parts - 1)]
    leaver = jnp.zeros((heads_here, DH), jnp.float32)
    for i in range(slots):
        top = fresh[i]
        for stat in stats:
            top = jnp.maximum(top, stat[:, i : i + 1])
        weight = jnp.exp(fresh[i] - top)
        total = weight
        mixed = weight.astype(jnp.bfloat16).astype(jnp.float32) * values[i]
        for k, stat in enumerate(stats):
            scale = jnp.exp(stat[:, i : i + 1] - top)
            block = part_ref[me, i] if k == 0 else landed[k - 1, i]
            total = total + scale * stat[:, slots + i : slots + i + 1]
            mixed = mixed + scale * block
        result = mixed / total
        leaver = jnp.where(leaving == i, result, leaver)
        for h in range(heads_here):
            flat[i : i + 1, h * DH : (h + 1) * DH] = result[h : h + 1]
    out_ref[...] = flat[...].astype(out_ref.dtype)
    row = jnp.concatenate([leaver[h : h + 1] for h in range(heads_here)], axis=1)
    leaver_ref[...] = row.astype(leaver_ref.dtype)


def finished(mig_slot, partials, mine, token_keys, token_values):
    parts, _, heads_here, _ = partials.shape
    slots = mine.shape[0]
    return pl.pallas_call(
        finish_kernel,
        out_shape=[
            jax.ShapeDtypeStruct((slots, heads_here * DH), jnp.bfloat16),
            jax.ShapeDtypeStruct((1, heads_here * DH), jnp.bfloat16),
        ],
        in_specs=[pl.BlockSpec(memory_space=pltpu.SMEM)]
        + [pl.BlockSpec(memory_space=pltpu.VMEM)] * 4,
        out_specs=[pl.BlockSpec(memory_space=pltpu.VMEM)] * 2,
        scratch_shapes=[
            pltpu.VMEM((slots, heads_here * DH), jnp.float32),
            pltpu.VMEM((parts - 1,) + partials.shape[1:], jnp.float32),
            pltpu.SemaphoreType.DMA((parts - 1,)),
            pltpu.SemaphoreType.DMA((parts - 1,)),
        ],
        compiler_params=pltpu.CompilerParams(
            collective_id=1, has_side_effects=True, vmem_limit_bytes=8 << 20
        ),
        cost_estimate=pl.CostEstimate(flops=0, bytes_accessed=8 << 20, transcendentals=0),
    )(mig_slot, partials, mine, token_keys, token_values)


def place_kernel(
    mig_ref, result_ref, row_ref, key_ref, value_ref, out_ref, kout_ref, vout_ref, kbuf, vbuf, sems
):
    pages = kbuf.shape[0]
    lanes = ((key_ref, kbuf, kout_ref), (value_ref, vbuf, vout_ref))
    span = 3 if pages % 3 == 0 else 1
    cuts = [pl.ds(j, span) for j in range(0, pages, span)]
    pairs = [(n, c) for c in range(len(cuts)) for n in range(2)]
    for n, c in pairs:
        source, buf, _ = lanes[n]
        pltpu.make_async_copy(source.at[cuts[c]], buf.at[cuts[c]], sems.at[n, c]).start()
    leaving = mig_ref[lax.axis_index("rep")]
    slot = lax.broadcasted_iota(jnp.int32, result_ref.shape, 0)
    row = row_ref[...].astype(jnp.float32)
    result = result_ref[...].astype(jnp.float32)
    out_ref[...] = jnp.where(slot == leaving, row, result).astype(out_ref.dtype)
    for n, c in pairs:
        source, buf, sink = lanes[n]
        pltpu.make_async_copy(source.at[cuts[c]], buf.at[cuts[c]], sems.at[n, c]).wait()
        pltpu.make_async_copy(buf.at[cuts[c]], sink.at[cuts[c]], sems.at[n, c]).start()
    for n, c in pairs:
        _, buf, sink = lanes[n]
        pltpu.make_async_copy(buf.at[cuts[c]], sink.at[cuts[c]], sems.at[n, c]).wait()


def placed_results(mig_slot, result, row, moved_keys, moved_values):
    moved = jax.ShapeDtypeStruct(moved_keys.shape, moved_keys.dtype)
    return pl.pallas_call(
        place_kernel,
        out_shape=[jax.ShapeDtypeStruct(result.shape, result.dtype), moved, moved],
        in_specs=[pl.BlockSpec(memory_space=pltpu.SMEM)]
        + [pl.BlockSpec(memory_space=pltpu.VMEM)] * 2
        + [pl.BlockSpec(memory_space=pl.ANY)] * 2,
        out_specs=[pl.BlockSpec(memory_space=pltpu.VMEM)]
        + [pl.BlockSpec(memory_space=pl.ANY)] * 2,
        scratch_shapes=[
            pltpu.VMEM(moved.shape, moved.dtype),
            pltpu.VMEM(moved.shape, moved.dtype),
            pltpu.SemaphoreType.DMA((2, moved.shape[0])),
        ],
        compiler_params=pltpu.CompilerParams(vmem_limit_bytes=8 << 20),
    )(mig_slot, result, row, moved_keys, moved_values)


def token_rows(fresh, parts, part_index):
    slots, width = fresh.shape
    heads_here = H // parts
    if width % DH == 0:
        return fresh.reshape(slots, width // DH, DH)
    every = lax.all_gather(fresh, "tp", axis=1, tiled=True).reshape(slots, KVH, DH)
    every = jnp.repeat(every, H // KVH, axis=1)
    return lax.dynamic_slice_in_dim(every, part_index * heads_here, heads_here, 1)


def body(
    queries, new_keys, new_values, key_pool, value_pool, lengths, page_table, mig_slot, mig_dst
):
    replicas = lax.axis_size("rep")
    parts = lax.axis_size("tp")
    here_rep = lax.axis_index("rep")
    part_index = lax.axis_index("tp")
    slots, _ = queries.shape
    k_width = new_keys.shape[1]
    heads_here = H // parts
    offset = mig_dst[0]
    start = (part_index * key_pool.shape[1]).reshape(1)
    visitor, keys_out, values_out = picked(
        page_table, mig_slot, queries, new_keys, new_values, key_pool, value_pool
    )

    def branch(distance):
        def run(visitor, keys_out, values_out):
            back = lax.ppermute(visitor, "rep", route_by(replicas, -distance))
            moved_keys = lax.ppermute(keys_out, "rep", route_by(replicas, distance))
            moved_values = lax.ppermute(values_out, "rep", route_by(replicas, distance))
            own_len = lax.dynamic_slice_in_dim(lengths, here_rep * slots, slots)
            tokens = jnp.concatenate([queries, new_keys, new_values], axis=1)
            tokens = tokens.reshape(slots, -1, DH)
            q_all, mine = shared(mig_slot, back, tokens, heads_here, parts)
            flat = mine[:, heads_here:].reshape(slots, 2 * k_width)
            token_keys = token_rows(flat[:, :k_width], parts, part_index)
            token_values = token_rows(flat[:, k_width:], parts, part_index)
            partials = attended_parts(
                page_table, own_len, start, q_all, key_pool, value_pool, parts
            )
            result, leaver = finished(mig_slot, partials, mine, token_keys, token_values)
            arrived = lax.ppermute(leaver, "rep", route_by(replicas, distance))
            return result, arrived, moved_keys, moved_values

        return run

    result, arrived, moved_keys, moved_values = lax.switch(
        offset - 1,
        [branch(distance) for distance in range(1, replicas)],
        visitor,
        keys_out,
        values_out,
    )
    return placed_results(mig_slot, result, arrived, moved_keys, moved_values)


def leaver_place(slots):
    return min(3, slots - 1)


def slot_at(place, leaving, spot):
    index = place - jnp.where(place > spot, 1, 0)
    other = index + jnp.where(index >= leaving, 1, 0)
    return jnp.where(place == spot, leaving, other)


def serve_kernel(
    distance,
    len_ref,
    mig_ref,
    table_ref,
    queries_ref,
    keys_ref,
    values_ref,
    key_hbm,
    value_hbm,
    out_ref,
    kout_ref,
    vout_ref,
    kpool,
    vpool,
    ksend,
    vsend,
    loose,
    q_ref,
    tokens_ref,
    q_all,
    visit,
    part,
    stats,
    early,
    landed,
    lstats,
    learly,
    row_out,
    row_in,
    flat,
    pool_sems,
    bulk_sems,
    visit_sems,
    share_sems,
    relay_sems,
    early_sems,
    late_sems,
    row_sems,
):
    pages, rows, width = kout_ref.shape
    slots, heads_here = q_ref.shape[:2]
    groups_here = (tokens_ref.shape[1] - heads_here) // 2
    replicas, parts = lax.axis_size("rep"), lax.axis_size("tp")
    rep, me = lax.axis_index("rep"), lax.axis_index("tp")
    spot = leaver_place(slots)
    group = H // KVH
    repeat = heads_here // groups_here
    page_len = rows * parts
    scaling = 1.0 / math.sqrt(DH)
    leaving = mig_ref[rep]
    ahead = lax.rem(rep + distance, replicas)
    behind = lax.rem(rep + replicas - distance, replicas)
    peers = [lax.rem(me + k, parts) for k in range(1, parts)]
    mesh_id = pl.DeviceIdType.MESH

    barrier = pltpu.get_barrier_semaphore()
    for other in (ahead, behind):
        pl.semaphore_signal(barrier, inc=1, device_id={"rep": other}, device_id_type=mesh_id)
    for peer in peers:
        pl.semaphore_signal(barrier, inc=1, device_id={"tp": peer}, device_id_type=mesh_id)

    loads = []
    cuts = pool_sems.shape[1]
    step = kpool.shape[0] // cuts
    for n, (source, target) in enumerate(((key_hbm, kpool), (value_hbm, vpool))):
        for c in range(cuts):
            cut = pl.ds(c * step, step)
            loads.append(
                pltpu.make_async_copy(source.at[cut], target.at[cut], pool_sems.at[n, c])
            )
    for copy in loads:
        copy.start()

    row_of = 0
    for ref in (queries_ref, keys_ref, values_ref):
        whole = ref[...].astype(jnp.float32)
        for h in range(ref.shape[1] // DH):
            loose[:, row_of, :] = whole[:, h * DH : (h + 1) * DH]
            row_of += 1
    for i in range(slots):
        token = loose[slot_at(i, leaving, spot)].astype(q_ref.dtype)
        tokens_ref[i] = token
        q_ref[i] = token[:heads_here]

    pl.semaphore_wait(barrier, parts + 1)

    def remote(source, target, sems, k, device):
        return pltpu.make_async_remote_copy(
            src_ref=source,
            dst_ref=target,
            send_sem=sems.at[0, k],
            recv_sem=sems.at[1, k],
            device_id=device,
            device_id_type=mesh_id,
        )

    visitor = remote(tokens_ref.at[spot], visit, visit_sems, 0, {"rep": behind})
    visitor.start()
    shares = []
    for k, peer in enumerate(peers):
        for n, cut in enumerate((pl.ds(0, spot), pl.ds(spot + 1, slots - spot - 1))):
            if cut.size:
                shares.append(
                    remote(
                        q_ref.at[cut], q_all.at[me, cut], share_sems, 2 * k + n, {"tp": peer}
                    )
                )
    for copy in shares:
        copy.start()
    q_all[me, 0:spot] = q_ref[0:spot]
    q_all[me, spot + 1 :] = q_ref[spot + 1 :]

    for copy in loads[:cuts]:
        copy.wait()
    blank = jnp.zeros((rows, width), ksend.dtype)

    def fill(target, pool):
        @pl.loop(0, pages)
        def _(j):
            page = table_ref[leaving, j]
            target[j] = jnp.where(page >= 0, pool[jnp.maximum(page, 0)], blank)

    fill(ksend, kpool)
    bulk_keys = remote(ksend, kout_ref, bulk_sems, 0, {"rep": ahead})
    bulk_keys.start()
    for copy in loads[cuts:]:
        copy.wait()
    fill(vsend, vpool)
    bulk_values = remote(vsend, vout_ref, bulk_sems, 1, {"rep": ahead})
    bulk_values.start()

    visitor.wait()
    relays = [
        remote(visit.at[pl.ds(0, heads_here)], q_all.at[me, spot], relay_sems, k, {"tp": peer})
        for k, peer in enumerate(peers)
    ]
    for copy in relays:
        copy.start()
    q_all[me, spot] = visit[0:heads_here]
    for copy in shares:
        copy.wait()

    head = lax.broadcasted_iota(jnp.int32, (H, DH), 0) // group
    column = lax.broadcasted_iota(jnp.int32, (heads_here, DH), 1)
    lane = lax.broadcasted_iota(jnp.int32, (H, pages * rows), 1)
    position = (lane // rows) * page_len + lane % rows + me * rows
    stats[...] = jnp.zeros_like(stats)

    early_copies = []
    for k, peer in enumerate(peers):
        early_copies.append(
            remote(part.at[peer, spot], landed.at[k, spot], early_sems, 2 * k, {"tp": peer})
        )
        early_copies.append(
            remote(early.at[peer], learly.at[k], early_sems, 2 * k + 1, {"tp": peer})
        )

    @pl.loop(0, slots)
    def _(i):
        @pl.when(i == spot)
        def _():
            for copy in relays:
                copy.wait()

        slot = slot_at(i, leaving, spot)
        length = len_ref[rep * slots + slot]

        def cached(pool):
            return jnp.concatenate(
                [pool[jnp.maximum(table_ref[slot, j], 0)] for j in range(pages)], axis=0
            )

        q = jnp.concatenate([q_all[t, i].astype(jnp.float32) for t in range(parts)], axis=0)
        spread = jnp.concatenate(
            [jnp.where(head == g, q, 0.0).astype(jnp.bfloat16) for g in range(KVH)], axis=1
        )
        scores = lax.dot_general(
            spread, cached(kpool), (((1,), (1,)), ((), ())), preferred_element_type=jnp.float32
        )
        usable = position < length
        masked = jnp.where(usable, scores * scaling, LOW)
        peak = jnp.max(masked, axis=1, keepdims=True)
        weights = jnp.where(usable, jnp.exp(masked - peak), 0.0)
        total = jnp.sum(weights, axis=1, keepdims=True)
        mixed = jnp.dot(
            weights.astype(jnp.bfloat16), cached(vpool), preferred_element_type=jnp.float32
        )
        own = jnp.concatenate(
            [mixed[g * group : (g + 1) * group, g * DH : (g + 1) * DH] for g in range(KVH)],
            axis=0,
        )
        for t in range(parts):
            cut = slice(t * heads_here, (t + 1) * heads_here)
            part[t, i] = own[cut]
            kept = jnp.where(column == i, peak[cut], stats[t])
            stats[t] = jnp.where(column == i + slots, total[cut], kept)

        @pl.when(i == spot)
        def _():
            early[...] = stats[...]
            for copy in early_copies:
                copy.start()

    late_copies = []
    for k, peer in enumerate(peers):
        for n, cut in enumerate((pl.ds(0, spot), pl.ds(spot + 1, slots - spot - 1))):
            if cut.size:
                late_copies.append(
                    remote(
                        part.at[peer, cut], landed.at[k, cut], late_sems, 3 * k + n, {"tp": peer}
                    )
                )
        late_copies.append(
            remote(stats.at[peer], lstats.at[k], late_sems, 3 * k + 2, {"tp": peer})
        )
    for copy in late_copies:
        copy.start()

    def over_groups(value):
        return jnp.concatenate(
            [jnp.broadcast_to(value[g : g + 1], (repeat, DH)) for g in range(groups_here)],
            axis=0,
        )

    def merged(i, token, rows_of_stats):
        token = token.astype(jnp.float32)
        keys = over_groups(token[heads_here : heads_here + groups_here])
        values = over_groups(token[heads_here + groups_here :])
        fresh = jnp.sum(token[:heads_here] * keys, axis=-1, keepdims=True) * scaling
        top = fresh
        for stat in rows_of_stats:
            top = jnp.maximum(top, stat[:, i : i + 1])
        weight = jnp.exp(fresh - top)
        total = weight
        mixed = weight.astype(jnp.bfloat16).astype(jnp.float32) * values
        for k, stat in enumerate(rows_of_stats):
            scale = jnp.exp(stat[:, i : i + 1] - top)
            block = part[me, i] if k == 0 else landed[k - 1, i]
            total = total + scale * stat[:, slots + i : slots + i + 1]
            mixed = mixed + scale * block
        return mixed / total

    for copy in early_copies:
        copy.wait()
    rows_of_stats = [early[me]] + [learly[k] for k in range(parts - 1)]
    row_out[...] = merged(spot, visit[...], rows_of_stats).astype(row_out.dtype)
    row = remote(row_out, row_in, row_sems, 0, {"rep": ahead})
    row.start()

    for copy in late_copies:
        copy.wait()
    rows_of_stats = [stats[me]] + [lstats[k] for k in range(parts - 1)]
    results = [
        merged(i, tokens_ref[i], rows_of_stats) if i != spot else None for i in range(slots)
    ]
    others = [r for r in results if r is not None]
    row.wait()
    arrived = row_in[...].astype(jnp.float32)
    for i in range(slots):
        before = others[i - 1] if i > 0 else arrived
        after = others[i] if i < slots - 1 else arrived
        value = jnp.where(leaving < i, before, after)
        value = jnp.where(leaving == i, arrived, value)
        for h in range(heads_here):
            flat[i : i + 1, h * DH : (h + 1) * DH] = value[h : h + 1]
    out_ref[...] = flat[...].astype(out_ref.dtype)
    bulk_keys.wait()
    bulk_values.wait()


def served(distance, lengths, mig_slot, table, queries, keys, values, key_pool, value_pool):
    slots, pages = table.shape
    rows, width = key_pool.shape[1:]
    parts = lax.axis_size("tp")
    heads_here = H // parts
    heads_all = heads_here + 2 * keys.shape[1] // DH
    others = parts - 1
    dtype = queries.dtype
    moved = (pages, rows, width)
    part = (slots, heads_here, DH)
    cuts = 2 if key_pool.shape[0] % 2 == 0 else 1
    return pl.pallas_call(
        functools.partial(serve_kernel, distance),
        out_shape=[
            jax.ShapeDtypeStruct(queries.shape, dtype),
            jax.ShapeDtypeStruct(moved, dtype),
            jax.ShapeDtypeStruct(moved, dtype),
        ],
        in_specs=[pl.BlockSpec(memory_space=pltpu.SMEM)] * 3
        + [pl.BlockSpec(memory_space=pltpu.VMEM)] * 3
        + [pl.BlockSpec(memory_space=pltpu.HBM)] * 2,
        out_specs=[pl.BlockSpec(memory_space=pltpu.VMEM)] * 3,
        scratch_shapes=[
            pltpu.VMEM(key_pool.shape, dtype),
            pltpu.VMEM(key_pool.shape, dtype),
            pltpu.VMEM(moved, dtype),
            pltpu.VMEM(moved, dtype),
            pltpu.VMEM((slots, heads_all, DH), jnp.float32),
            pltpu.VMEM(part, dtype),
            pltpu.VMEM((slots, heads_all, DH), dtype),
            pltpu.VMEM((parts,) + part, dtype),
            pltpu.VMEM((heads_all, DH), dtype),
            pltpu.VMEM((parts,) + part, jnp.float32),
            pltpu.VMEM((parts, heads_here, DH), jnp.float32),
            pltpu.VMEM((parts, heads_here, DH), jnp.float32),
            pltpu.VMEM((others,) + part, jnp.float32),
            pltpu.VMEM((others, heads_here, DH), jnp.float32),
            pltpu.VMEM((others, heads_here, DH), jnp.float32),
            pltpu.VMEM((heads_here, DH), dtype),
            pltpu.VMEM((heads_here, DH), dtype),
            pltpu.VMEM((slots, heads_here * DH), jnp.float32),
            pltpu.SemaphoreType.DMA((2, cuts)),
            pltpu.SemaphoreType.DMA((2, 2)),
            pltpu.SemaphoreType.DMA((2, 1)),
            pltpu.SemaphoreType.DMA((2, 2 * others)),
            pltpu.SemaphoreType.DMA((2, others)),
            pltpu.SemaphoreType.DMA((2, 2 * others)),
            pltpu.SemaphoreType.DMA((2, 3 * others)),
            pltpu.SemaphoreType.DMA((2, 1)),
        ],
        compiler_params=pltpu.CompilerParams(
            collective_id=2 + distance, has_side_effects=True, vmem_limit_bytes=32 << 20
        ),
        cost_estimate=pl.CostEstimate(
            flops=4 * H * slots * pages * rows * width,
            bytes_accessed=4 * math.prod(key_pool.shape),
            transcendentals=0,
        ),
    )(lengths, mig_slot, table, queries, keys, values, key_pool, value_pool)


def settle_kernel(result_ref, key_ref, value_ref, out_ref, kout_ref, vout_ref, sems):
    copies = [
        pltpu.make_async_copy(source, target, sems.at[n])
        for n, (source, target) in enumerate(
            ((key_ref, kout_ref), (value_ref, vout_ref), (result_ref, out_ref))
        )
    ]
    for copy in copies:
        copy.start()
    for copy in copies:
        copy.wait()


def settled(*arrays):
    return pl.pallas_call(
        settle_kernel,
        out_shape=[jax.ShapeDtypeStruct(a.shape, a.dtype) for a in arrays],
        in_specs=[pl.BlockSpec(memory_space=pltpu.VMEM)] * 3,
        out_specs=[pl.BlockSpec(memory_space=pltpu.HBM)] * 3,
        scratch_shapes=[pltpu.SemaphoreType.DMA((3,))],
        compiler_params=pltpu.CompilerParams(vmem_limit_bytes=8 << 20),
    )(*arrays)


def swift_body(
    queries, new_keys, new_values, key_pool, value_pool, lengths, page_table, mig_slot, mig_dst
):
    replicas = lax.axis_size("rep")
    results = lax.switch(
        mig_dst[0] - 1,
        [functools.partial(served, distance) for distance in range(1, replicas)],
        lengths,
        mig_slot,
        page_table,
        queries,
        new_keys,
        new_values,
        key_pool,
        value_pool,
    )
    return settled(*results)


def solution(mesh):
    placed = (
        P("rep", "tp"),
        P("rep", "tp"),
        P("rep", "tp"),
        P("rep", "tp", None),
        P("rep", "tp", None),
        P(),
        P("rep", None),
        P(),
        P(),
    )
    swift = KVH % mesh.shape["tp"] == 0
    return jax.shard_map(
        swift_body if swift else body,
        mesh=mesh,
        in_specs=placed,
        out_specs=(P("rep", "tp"), P("rep", "tp", None), P("rep", "tp", None)),
        check_vma=False,
    )
```

```python
import functools
import math


import jax
import jax.numpy as jnp
from jax import lax
from jax.experimental import pallas as pl
from jax.experimental.pallas import tpu as pltpu
from jax.sharding import PartitionSpec as P

H = 64
KVH = 8
DH = 128
LOW = -1e30


def route_by(count, distance):
    return [(i, (i + distance) % count) for i in range(count)]


def pick_kernel(
    table_ref, mig_ref, q_ref, nk_ref, nv_ref, key_ref, value_ref, row_ref, kout_ref, vout_ref, sems
):
    pages = kout_ref.shape[0]
    leaving = mig_ref[lax.axis_index("rep")]

    @pl.loop(0, pages)
    def _(j):
        page = jnp.maximum(table_ref[leaving, j], 0)
        pltpu.make_async_copy(key_ref.at[page], kout_ref.at[j], sems.at[0]).start()
        pltpu.make_async_copy(value_ref.at[page], vout_ref.at[j], sems.at[1]).start()

    at = 0
    for ref in (q_ref, nk_ref, nv_ref):
        width = ref.shape[1]
        slot = lax.broadcasted_iota(jnp.int32, ref.shape, 0)
        chosen = jnp.where(slot == leaving, ref[...].astype(jnp.float32), 0.0)
        row = jnp.sum(chosen, axis=0, keepdims=True)
        row_ref[:, at : at + width] = row.astype(jnp.bfloat16)
        at += width
    pltpu.make_async_copy(key_ref.at[pl.ds(0, pages)], kout_ref, sems.at[0]).wait()
    pltpu.make_async_copy(value_ref.at[pl.ds(0, pages)], vout_ref, sems.at[1]).wait()

    @pl.loop(0, pages)
    def _(j):
        @pl.when(table_ref[leaving, j] < 0)
        def _():
            kout_ref[j] = jnp.zeros(kout_ref.shape[1:], kout_ref.dtype)
            vout_ref[j] = jnp.zeros(vout_ref.shape[1:], vout_ref.dtype)


def picked(table, mig_slot, queries, new_keys, new_values, key_pool, value_pool):
    shape = (table.shape[1],) + key_pool.shape[1:]
    width = queries.shape[1] + 2 * new_keys.shape[1]
    return pl.pallas_call(
        pick_kernel,
        out_shape=[
            jax.ShapeDtypeStruct((1, width), jnp.bfloat16),
            jax.ShapeDtypeStruct(shape, key_pool.dtype),
            jax.ShapeDtypeStruct(shape, key_pool.dtype),
        ],
        in_specs=[pl.BlockSpec(memory_space=pltpu.SMEM)] * 2
        + [pl.BlockSpec(memory_space=pltpu.VMEM)] * 3
        + [pl.BlockSpec(memory_space=pl.ANY)] * 2,
        out_specs=[pl.BlockSpec(memory_space=pltpu.VMEM)] * 3,
        scratch_shapes=[pltpu.SemaphoreType.DMA((2,))],
        compiler_params=pltpu.CompilerParams(vmem_limit_bytes=8 << 20),
        cost_estimate=pl.CostEstimate(
            flops=0, bytes_accessed=8 * math.prod(shape), transcendentals=0
        ),
    )(table, mig_slot, queries, new_keys, new_values, key_pool, value_pool)


def greet(parts):
    me = lax.axis_index("tp")
    barrier = pltpu.get_barrier_semaphore()
    for k in range(1, parts):
        pl.semaphore_signal(
            barrier,
            inc=1,
            device_id={"tp": lax.rem(me + k, parts)},
            device_id_type=pl.DeviceIdType.MESH,
        )
    pl.semaphore_wait(barrier, parts - 1)
    return me


def share_kernel(mig_ref, back_ref, tokens_ref, all_ref, mine_ref, own, send_sems, recv_sems):
    parts, slots, heads_here, _ = all_ref.shape
    chunks = tokens_ref.shape[1]
    leaving = mig_ref[lax.axis_index("rep")]
    back = back_ref[...].astype(jnp.float32)
    row = jnp.concatenate([back[:, h * DH : (h + 1) * DH] for h in range(chunks)], axis=0)
    for i in range(slots):
        value = jnp.where(leaving == i, row, tokens_ref[i].astype(jnp.float32))
        value = value.astype(jnp.bfloat16)
        mine_ref[i] = value
        own[i] = value[:heads_here]
    me = greet(parts)
    copies = []
    for k in range(1, parts):
        copy = pltpu.make_async_remote_copy(
            src_ref=own,
            dst_ref=all_ref.at[me],
            send_sem=send_sems.at[k - 1],
            recv_sem=recv_sems.at[k - 1],
            device_id={"tp": lax.rem(me + k, parts)},
            device_id_type=pl.DeviceIdType.MESH,
        )
        copy.start()
        copies.append(copy)
    all_ref[me] = own[...]
    for copy in copies:
        copy.wait()


def shared(mig_slot, back, tokens, heads_here, parts):
    slots = tokens.shape[0]
    return pl.pallas_call(
        share_kernel,
        out_shape=[
            jax.ShapeDtypeStruct((parts, slots, heads_here, DH), jnp.bfloat16),
            jax.ShapeDtypeStruct(tokens.shape, jnp.bfloat16),
        ],
        in_specs=[pl.BlockSpec(memory_space=pltpu.SMEM)]
        + [pl.BlockSpec(memory_space=pltpu.VMEM)] * 2,
        out_specs=[pl.BlockSpec(memory_space=pltpu.VMEM)] * 2,
        scratch_shapes=[
            pltpu.VMEM((slots, heads_here, DH), jnp.bfloat16),
            pltpu.SemaphoreType.DMA((parts - 1,)),
            pltpu.SemaphoreType.DMA((parts - 1,)),
        ],
        compiler_params=pltpu.CompilerParams(
            collective_id=0, has_side_effects=True, vmem_limit_bytes=8 << 20
        ),
        cost_estimate=pl.CostEstimate(flops=0, bytes_accessed=8 << 20, transcendentals=0),
    )(mig_slot, back, tokens)


def flat_rows(block):
    pages, rows, width = block.shape
    if rows % 16 == 0:
        return block.reshape(pages * rows, width)
    return block.astype(jnp.float32).reshape(pages * rows, width).astype(block.dtype)


def attend_kernel(
    table_ref,
    len_ref,
    start_ref,
    q_ref,
    key_ref,
    value_ref,
    out_ref,
    kbuf,
    vbuf,
    stats_ref,
    ksem,
    vsem,
):
    slots, pages, rows, width = kbuf.shape
    parts, heads_here = q_ref.shape[0], q_ref.shape[2]
    group = H // KVH
    page_len = rows * parts
    scaling = 1.0 / math.sqrt(DH)
    steps = 3 if pages % 3 == 0 else 1
    step_pages = pages // steps

    def live_pages(i):
        return lax.div(len_ref[i] + (page_len - 1), page_len)

    def key_copy(i, j):
        page = jnp.maximum(table_ref[i, j], 0)
        return pltpu.make_async_copy(key_ref.at[page], kbuf.at[i, j], ksem.at[i, j])

    def value_copy(i, j):
        page = jnp.maximum(table_ref[i, j], 0)
        return pltpu.make_async_copy(value_ref.at[page], vbuf.at[i, j], vsem.at[i, j])

    @pl.loop(0, slots)
    def _(i):
        @pl.loop(0, live_pages(i))
        def _(j):
            key_copy(i, j).start()
            value_copy(i, j).start()

    head = lax.broadcasted_iota(jnp.int32, (H, DH), 0) // group
    column = lax.broadcasted_iota(jnp.int32, (H, DH), 1)
    stats_ref[...] = jnp.zeros_like(stats_ref)

    def attend(i, used):
        tokens = used * rows
        lane = lax.broadcasted_iota(jnp.int32, (H, tokens), 1)
        position = (lane // rows) * page_len + lane % rows + start_ref[0]
        q = jnp.concatenate([q_ref[t, i].astype(jnp.float32) for t in range(parts)], axis=0)
        spread = jnp.concatenate(
            [jnp.where(head == g, q, 0.0).astype(jnp.bfloat16) for g in range(KVH)], axis=1
        )
        scores = lax.dot_general(
            spread,
            flat_rows(kbuf[i, 0:used]),
            (((1,), (1,)), ((), ())),
            preferred_element_type=jnp.float32,
        )
        usable = position < len_ref[i]
        masked = jnp.where(usable, scores * scaling, LOW)
        peak = jnp.max(masked, axis=1, keepdims=True)
        weights = jnp.where(usable, jnp.exp(masked - peak), 0.0)
        total = jnp.sum(weights, axis=1, keepdims=True)
        mixed = jnp.dot(
            weights.astype(jnp.bfloat16),
            flat_rows(vbuf[i, 0:used]),
            preferred_element_type=jnp.float32,
        )
        own = jnp.concatenate(
            [
                mixed[g * group : (g + 1) * group, g * DH : (g + 1) * DH]
                for g in range(KVH)
            ],
            axis=0,
        )
        for t in range(parts):
            out_ref[t, i] = own[t * heads_here : (t + 1) * heads_here]
        stats = jnp.where(column == i, peak, stats_ref[...])
        stats_ref[...] = jnp.where(column == i + slots, total, stats)

    @pl.loop(0, slots)
    def _(i):
        live = live_pages(i)
        needed = lax.div(live + (step_pages - 1), step_pages)

        @pl.loop(live, needed * step_pages)
        def _(j):
            vbuf[i, j] = jnp.zeros((rows, width), vbuf.dtype)

        @pl.loop(0, live)
        def _(j):
            key_copy(i, j).wait()
            value_copy(i, j).wait()

        for step in range(1, steps + 1):

            @pl.when(needed == step)
            def _():
                attend(i, step * step_pages)

    for t in range(parts):
        out_ref[t, slots] = stats_ref[t * heads_here : (t + 1) * heads_here]


def attended_parts(table, lens, start, q, key_pool, value_pool, parts):
    slots, pages = table.shape
    rows, width = key_pool.shape[1:]
    buffer = (slots, pages, rows, width)
    return pl.pallas_call(
        attend_kernel,
        out_shape=jax.ShapeDtypeStruct((parts, slots + 1, H // parts, DH), jnp.float32),
        in_specs=[pl.BlockSpec(memory_space=pltpu.SMEM)] * 3
        + [pl.BlockSpec(memory_space=pltpu.VMEM)]
        + [pl.BlockSpec(memory_space=pl.ANY)] * 2,
        out_specs=pl.BlockSpec(memory_space=pltpu.VMEM),
        scratch_shapes=[
            pltpu.VMEM(buffer, key_pool.dtype),
            pltpu.VMEM(buffer, value_pool.dtype),
            pltpu.VMEM((H, DH), jnp.float32),
            pltpu.SemaphoreType.DMA((slots, pages)),
            pltpu.SemaphoreType.DMA((slots, pages)),
        ],
        compiler_params=pltpu.CompilerParams(vmem_limit_bytes=24 << 20),
        cost_estimate=pl.CostEstimate(
            flops=4 * H * pages * rows * width * slots,
            bytes_accessed=4 * math.prod(buffer),
            transcendentals=0,
        ),
    )(table, lens, start, q, key_pool, value_pool)


def finish_kernel(
    mig_ref,
    part_ref,
    mine_ref,
    tk_ref,
    tv_ref,
    out_ref,
    leaver_ref,
    flat,
    landed,
    send_sems,
    recv_sems,
):
    parts, _, heads_here, _ = part_ref.shape
    slots = mine_ref.shape[0]
    repeat = heads_here // tk_ref.shape[1]
    leaving = mig_ref[lax.axis_index("rep")]
    scaling = 1.0 / math.sqrt(DH)
    me = greet(parts)
    copies = []
    for k in range(1, parts):
        peer = lax.rem(me + k, parts)
        copy = pltpu.make_async_remote_copy(
            src_ref=part_ref.at[peer],
            dst_ref=landed.at[k - 1],
            send_sem=send_sems.at[k - 1],
            recv_sem=recv_sems.at[k - 1],
            device_id={"tp": peer},
            device_id_type=pl.DeviceIdType.MESH,
        )
        copy.start()
        copies.append(copy)

    def spread(ref, i):
        value = ref[i].astype(jnp.float32)
        return jnp.concatenate(
            [
                jnp.broadcast_to(value[g : g + 1], (repeat, DH))
                for g in range(value.shape[0])
            ],
            axis=0,
        )

    fresh, values = [], []
    for i in range(slots):
        q = mine_ref[i].astype(jnp.float32)[:heads_here]
        fresh.append(jnp.sum(q * spread(tk_ref, i), axis=-1, keepdims=True) * scaling)
        values.append(spread(tv_ref, i))
    for copy in copies:
        copy.wait()
    stats = [part_ref[me, slots]] + [landed[k, slots] for k in range(parts - 1)]
    leaver = jnp.zeros((heads_here, DH), jnp.float32)
    for i in range(slots):
        top = fresh[i]
        for stat in stats:
            top = jnp.maximum(top, stat[:, i : i + 1])
        weight = jnp.exp(fresh[i] - top)
        total = weight
        mixed = weight.astype(jnp.bfloat16).astype(jnp.float32) * values[i]
        for k, stat in enumerate(stats):
            scale = jnp.exp(stat[:, i : i + 1] - top)
            block = part_ref[me, i] if k == 0 else landed[k - 1, i]
            total = total + scale * stat[:, slots + i : slots + i + 1]
            mixed = mixed + scale * block
        result = mixed / total
        leaver = jnp.where(leaving == i, result, leaver)
        for h in range(heads_here):
            flat[i : i + 1, h * DH : (h + 1) * DH] = result[h : h + 1]
    out_ref[...] = flat[...].astype(out_ref.dtype)
    row = jnp.concatenate([leaver[h : h + 1] for h in range(heads_here)], axis=1)
    leaver_ref[...] = row.astype(leaver_ref.dtype)


def finished(mig_slot, partials, mine, token_keys, token_values):
    parts, _, heads_here, _ = partials.shape
    slots = mine.shape[0]
    return pl.pallas_call(
        finish_kernel,
        out_shape=[
            jax.ShapeDtypeStruct((slots, heads_here * DH), jnp.bfloat16),
            jax.ShapeDtypeStruct((1, heads_here * DH), jnp.bfloat16),
        ],
        in_specs=[pl.BlockSpec(memory_space=pltpu.SMEM)]
        + [pl.BlockSpec(memory_space=pltpu.VMEM)] * 4,
        out_specs=[pl.BlockSpec(memory_space=pltpu.VMEM)] * 2,
        scratch_shapes=[
            pltpu.VMEM((slots, heads_here * DH), jnp.float32),
            pltpu.VMEM((parts - 1,) + partials.shape[1:], jnp.float32),
            pltpu.SemaphoreType.DMA((parts - 1,)),
            pltpu.SemaphoreType.DMA((parts - 1,)),
        ],
        compiler_params=pltpu.CompilerParams(
            collective_id=1, has_side_effects=True, vmem_limit_bytes=8 << 20
        ),
        cost_estimate=pl.CostEstimate(flops=0, bytes_accessed=8 << 20, transcendentals=0),
    )(mig_slot, partials, mine, token_keys, token_values)


def place_kernel(
    mig_ref, result_ref, row_ref, key_ref, value_ref, out_ref, kout_ref, vout_ref, kbuf, vbuf, sems
):
    pages = kbuf.shape[0]
    lanes = ((key_ref, kbuf, kout_ref), (value_ref, vbuf, vout_ref))
    span = 3 if pages % 3 == 0 else 1
    cuts = [pl.ds(j, span) for j in range(0, pages, span)]
    pairs = [(n, c) for c in range(len(cuts)) for n in range(2)]
    for n, c in pairs:
        source, buf, _ = lanes[n]
        pltpu.make_async_copy(source.at[cuts[c]], buf.at[cuts[c]], sems.at[n, c]).start()
    leaving = mig_ref[lax.axis_index("rep")]
    slot = lax.broadcasted_iota(jnp.int32, result_ref.shape, 0)
    row = row_ref[...].astype(jnp.float32)
    result = result_ref[...].astype(jnp.float32)
    out_ref[...] = jnp.where(slot == leaving, row, result).astype(out_ref.dtype)
    for n, c in pairs:
        source, buf, sink = lanes[n]
        pltpu.make_async_copy(source.at[cuts[c]], buf.at[cuts[c]], sems.at[n, c]).wait()
        pltpu.make_async_copy(buf.at[cuts[c]], sink.at[cuts[c]], sems.at[n, c]).start()
    for n, c in pairs:
        _, buf, sink = lanes[n]
        pltpu.make_async_copy(buf.at[cuts[c]], sink.at[cuts[c]], sems.at[n, c]).wait()


def placed_results(mig_slot, result, row, moved_keys, moved_values):
    moved = jax.ShapeDtypeStruct(moved_keys.shape, moved_keys.dtype)
    return pl.pallas_call(
        place_kernel,
        out_shape=[jax.ShapeDtypeStruct(result.shape, result.dtype), moved, moved],
        in_specs=[pl.BlockSpec(memory_space=pltpu.SMEM)]
        + [pl.BlockSpec(memory_space=pltpu.VMEM)] * 2
        + [pl.BlockSpec(memory_space=pl.ANY)] * 2,
        out_specs=[pl.BlockSpec(memory_space=pltpu.VMEM)]
        + [pl.BlockSpec(memory_space=pl.ANY)] * 2,
        scratch_shapes=[
            pltpu.VMEM(moved.shape, moved.dtype),
            pltpu.VMEM(moved.shape, moved.dtype),
            pltpu.SemaphoreType.DMA((2, moved.shape[0])),
        ],
        compiler_params=pltpu.CompilerParams(vmem_limit_bytes=8 << 20),
    )(mig_slot, result, row, moved_keys, moved_values)


def token_rows(fresh, parts, part_index):
    slots, width = fresh.shape
    heads_here = H // parts
    if width % DH == 0:
        return fresh.reshape(slots, width // DH, DH)
    every = lax.all_gather(fresh, "tp", axis=1, tiled=True).reshape(slots, KVH, DH)
    every = jnp.repeat(every, H // KVH, axis=1)
    return lax.dynamic_slice_in_dim(every, part_index * heads_here, heads_here, 1)


def body(
    queries, new_keys, new_values, key_pool, value_pool, lengths, page_table, mig_slot, mig_dst
):
    replicas = lax.axis_size("rep")
    parts = lax.axis_size("tp")
    here_rep = lax.axis_index("rep")
    part_index = lax.axis_index("tp")
    slots, _ = queries.shape
    k_width = new_keys.shape[1]
    heads_here = H // parts
    offset = mig_dst[0]
    start = (part_index * key_pool.shape[1]).reshape(1)
    visitor, keys_out, values_out = picked(
        page_table, mig_slot, queries, new_keys, new_values, key_pool, value_pool
    )

    def branch(distance):
        def run(visitor, keys_out, values_out):
            back = lax.ppermute(visitor, "rep", route_by(replicas, -distance))
            moved_keys = lax.ppermute(keys_out, "rep", route_by(replicas, distance))
            moved_values = lax.ppermute(values_out, "rep", route_by(replicas, distance))
            own_len = lax.dynamic_slice_in_dim(lengths, here_rep * slots, slots)
            tokens = jnp.concatenate([queries, new_keys, new_values], axis=1)
            tokens = tokens.reshape(slots, -1, DH)
            q_all, mine = shared(mig_slot, back, tokens, heads_here, parts)
            flat = mine[:, heads_here:].reshape(slots, 2 * k_width)
            token_keys = token_rows(flat[:, :k_width], parts, part_index)
            token_values = token_rows(flat[:, k_width:], parts, part_index)
            partials = attended_parts(
                page_table, own_len, start, q_all, key_pool, value_pool, parts
            )
            result, leaver = finished(mig_slot, partials, mine, token_keys, token_values)
            arrived = lax.ppermute(leaver, "rep", route_by(replicas, distance))
            return result, arrived, moved_keys, moved_values

        return run

    result, arrived, moved_keys, moved_values = lax.switch(
        offset - 1,
        [branch(distance) for distance in range(1, replicas)],
        visitor,
        keys_out,
        values_out,
    )
    return placed_results(mig_slot, result, arrived, moved_keys, moved_values)


def leaver_place(slots):
    return min(3, slots - 1)


def crossing(replicas, distance):
    cuts = {}
    for source in range(replicas):
        start, end = source // 2, (source + distance) % replicas // 2
        for chip in range(min(start, end), max(start, end)):
            cuts.setdefault((chip, end > start), []).append(source)
    return cuts


def paired_sources(replicas, distance):
    cuts = crossing(replicas, distance).values()
    most = max(map(len, cuts))
    busiest = [flows for flows in cuts if len(flows) == most]
    return [
        s for s in range(replicas) if any(s in flows and s ^ 1 in flows for flows in busiest)
    ]


def passing(replicas, distance):
    return sorted(set(sum(crossing(replicas, distance).values(), [])))


def room_choices(replicas, distance, pages):
    if replicas % 2:
        return [pages]
    if paired_sources(replicas, distance):
        return [8, 10, 12]
    return [pages]


def among(index, members):
    found = index < 0
    for member in members:
        found = found | (index == member)
    return found


def slot_at(place, leaving, spot):
    index = place - jnp.where(place > spot, 1, 0)
    other = index + jnp.where(index >= leaving, 1, 0)
    return jnp.where(place == spot, leaving, other)


def serve_kernel(
    distance,
    room,
    len_hbm,
    mig_hbm,
    table_hbm,
    queries_hbm,
    keys_hbm,
    values_hbm,
    key_hbm,
    value_hbm,
    out_ref,
    kout_ref,
    vout_ref,
    len_ref,
    mig_ref,
    table_ref,
    queries_ref,
    keys_ref,
    values_ref,
    kpool,
    vpool,
    ksend,
    vsend,
    kguest,
    vguest,
    loose,
    q_ref,
    tokens_ref,
    q_all,
    visit,
    part,
    stats,
    early,
    landed,
    lstats,
    learly,
    row_out,
    row_in,
    done,
    ordered,
    small_sems,
    pool_sems,
    bulk_sems,
    post_sems,
    visit_sems,
    share_sems,
    relay_sems,
    early_sems,
    late_sems,
    row_sems,
):
    pages, rows, _ = kout_ref.shape
    slots, heads_here = q_ref.shape[:2]
    groups_here = (tokens_ref.shape[1] - heads_here) // 2
    replicas, parts = lax.axis_size("rep"), lax.axis_size("tp")
    rep, me = lax.axis_index("rep"), lax.axis_index("tp")
    spot = leaver_place(slots)
    group = H // KVH
    repeat = heads_here // groups_here
    page_len = rows * parts
    scaling = 1.0 / math.sqrt(DH)
    ahead = lax.rem(rep + distance, replicas)
    behind = lax.rem(rep + replicas - distance, replicas)
    peers = [lax.rem(me + k, parts) for k in range(1, parts)]
    mesh_id = pl.DeviceIdType.MESH

    alone = not paired_sources(replicas, distance)
    extra = 0 if alone else pages - room
    members = paired_sources(replicas, distance) if extra else []
    sends_paired = among(rep, members)
    gets_paired = among(behind, members)
    partner = rep + 1 - 2 * lax.rem(rep, 2)
    mate = lax.rem(behind + 1 - 2 * lax.rem(behind, 2) + distance, replicas)

    barrier = pltpu.get_barrier_semaphore()

    def greet_rep(other):
        pl.semaphore_signal(barrier, inc=1, device_id={"rep": other}, device_id_type=mesh_id)

    for other in (ahead, behind):
        greet_rep(other)
    for peer in peers:
        pl.semaphore_signal(barrier, inc=1, device_id={"tp": peer}, device_id_type=mesh_id)
    if extra:
        greet_rep(partner)
        if distance % 2:
            greet_rep(mate)

    smalls = [
        pltpu.make_async_copy(source, target, small_sems.at[n])
        for n, (source, target) in enumerate(
            (
                (table_hbm, table_ref),
                (mig_hbm, mig_ref),
                (len_hbm, len_ref),
                (queries_hbm, queries_ref),
                (keys_hbm, keys_ref),
                (values_hbm, values_ref),
            )
        )
    ]
    for copy in smalls:
        copy.start()
    loads = []
    cuts = pool_sems.shape[1]
    step = kpool.shape[0] // cuts
    for n, (source, target) in enumerate(((key_hbm, kpool), (value_hbm, vpool))):
        for c in range(cuts):
            cut = pl.ds(c * step, step)
            loads.append(
                pltpu.make_async_copy(source.at[cut], target.at[cut], pool_sems.at[n, c])
            )
    for copy in loads[:cuts]:
        copy.start()

    for copy in smalls:
        copy.wait()
    leaving = mig_ref[rep]
    row_of = 0
    for ref in (queries_ref, keys_ref, values_ref):
        whole = ref[...].astype(jnp.float32)
        for h in range(ref.shape[1] // DH):
            loose[:, row_of, :] = whole[:, h * DH : (h + 1) * DH]
            row_of += 1
    for i in range(slots):
        token = loose[slot_at(i, leaving, spot)].astype(q_ref.dtype)
        tokens_ref[i] = token
        q_ref[i] = token[:heads_here]

    pl.semaphore_wait(barrier, parts + 1 + (1 + distance % 2 if extra else 0))

    def remote(source, target, sems, k, device):
        return pltpu.make_async_remote_copy(
            src_ref=source,
            dst_ref=target,
            send_sem=sems.at[0, k],
            recv_sem=sems.at[1, k],
            device_id=device,
            device_id_type=mesh_id,
        )

    visitor = remote(tokens_ref.at[spot], visit, visit_sems, 0, {"rep": behind})
    visitor.start()
    shares = []
    for k, peer in enumerate(peers):
        for n, cut in enumerate((pl.ds(0, spot), pl.ds(spot + 1, slots - spot - 1))):
            if cut.size:
                shares.append(
                    remote(
                        q_ref.at[cut], q_all.at[me, cut], share_sems, 2 * k + n, {"tp": peer}
                    )
                )
    for copy in shares:
        copy.start()
    q_all[me, 0:spot] = q_ref[0:spot]
    q_all[me, spot + 1 :] = q_ref[spot + 1 :]

    main = room - extra
    first = min(2, main)
    to_ahead, to_partner, to_mate = {"rep": ahead}, {"rep": partner}, {"rep": mate}
    lanes = ((ksend, kguest, kout_ref), (vsend, vguest, vout_ref))

    def cut_copy(n, kind, low, high):
        source, _, target = lanes[n]
        cut = pl.ds(low, high - low)
        return remote(source.at[cut], target.at[cut], bulk_sems, 2 * kind + n, to_ahead)

    plain = [cut_copy(n, 0, 0, room if alone else pages) for n in range(2)]
    opening, shared_out, closing, swaps, posts = [], [], [], [], []
    if extra:
        if first:
            opening = [cut_copy(n, 1, 0, first) for n in range(2)]
        shared_out = [cut_copy(n, 2, main, room) for n in range(2)]
        if main > first:
            closing = [cut_copy(n, 3, first, main) for n in range(2)]
        for n, (source, guest, target) in enumerate(lanes):
            swaps.append(
                remote(source.at[pl.ds(room, extra)], guest, bulk_sems, 8 + n, to_partner)
            )
            for i in range(extra):
                posts.append(
                    remote(
                        target.at[room - 1 - i],
                        target.at[room + i],
                        post_sems,
                        n * extra + i,
                        to_mate,
                    )
                )

    def fill(target, pool):
        @pl.loop(0, pages)
        def _(j):
            target[j] = pool[jnp.maximum(table_ref[leaving, j], 0)]

    for n, pool in enumerate((kpool, vpool)):
        for copy in loads[n * cuts : (n + 1) * cuts]:
            copy.wait()
        if n == 0:
            for copy in loads[cuts:]:
                copy.start()
        fill(lanes[n][0], pool)
        if extra:

            @pl.when(sends_paired)
            def _():
                swaps[n].start()
                if opening:
                    opening[n].start()

            pl.when(jnp.logical_not(sends_paired))(plain[n].start)
        else:
            plain[n].start()

    visitor.wait()
    relays = [
        remote(visit.at[pl.ds(0, heads_here)], q_all.at[me, spot], relay_sems, k, {"tp": peer})
        for k, peer in enumerate(peers)
    ]
    for copy in relays:
        copy.start()
    q_all[me, spot] = visit[0:heads_here]
    for copy in shares:
        copy.wait()

    if extra:

        @pl.when(sends_paired)
        def _():
            theirs = len_ref[partner * slots + mig_ref[partner]]
            for n, (source, guest, _) in enumerate(lanes):
                swaps[n].wait()
                for i in range(extra):
                    spare = room - 1 - i
                    source[spare] = jnp.where(
                        theirs > (room + i) * page_len, guest[i], source[spare]
                    )
                shared_out[n].start()
            for copy in closing:
                copy.start()

    head = lax.broadcasted_iota(jnp.int32, (H, DH), 0) // group
    column = lax.broadcasted_iota(jnp.int32, (heads_here, DH), 1)
    lane = lax.broadcasted_iota(jnp.int32, (H, pages * rows), 1)
    position = (lane // rows) * page_len + lane % rows + me * rows
    stats[...] = jnp.zeros_like(stats)

    early_copies = []
    for k, peer in enumerate(peers):
        early_copies.append(
            remote(part.at[peer, spot], landed.at[k, spot], early_sems, 2 * k, {"tp": peer})
        )
        early_copies.append(
            remote(early.at[peer], learly.at[k], early_sems, 2 * k + 1, {"tp": peer})
        )

    @pl.loop(0, slots)
    def _(i):
        @pl.when(i == spot)
        def _():
            for copy in relays:
                copy.wait()

        slot = slot_at(i, leaving, spot)
        length = len_ref[rep * slots + slot]

        def cached(pool):
            return jnp.concatenate(
                [pool[jnp.maximum(table_ref[slot, j], 0)] for j in range(pages)], axis=0
            )

        q = jnp.concatenate([q_all[t, i].astype(jnp.float32) for t in range(parts)], axis=0)
        spread = jnp.concatenate(
            [jnp.where(head == g, q, 0.0).astype(jnp.bfloat16) for g in range(KVH)], axis=1
        )
        scores = lax.dot_general(
            spread, cached(kpool), (((1,), (1,)), ((), ())), preferred_element_type=jnp.float32
        )
        usable = position < length
        masked = jnp.where(usable, scores * scaling, LOW)
        peak = jnp.max(masked, axis=1, keepdims=True)
        weights = jnp.where(usable, jnp.exp(masked - peak), 0.0)
        total = jnp.sum(weights, axis=1, keepdims=True)
        mixed = jnp.dot(
            weights.astype(jnp.bfloat16), cached(vpool), preferred_element_type=jnp.float32
        )
        own = jnp.concatenate(
            [mixed[g * group : (g + 1) * group, g * DH : (g + 1) * DH] for g in range(KVH)],
            axis=0,
        )
        for t in range(parts):
            cut = slice(t * heads_here, (t + 1) * heads_here)
            part[t, i] = own[cut]
            kept = jnp.where(column == i, peak[cut], stats[t])
            stats[t] = jnp.where(column == i + slots, total[cut], kept)

        @pl.when(i == spot)
        def _():
            early[...] = stats[...]
            for copy in early_copies:
                copy.start()

    late_copies = []
    for k, peer in enumerate(peers):
        for n, cut in enumerate((pl.ds(0, spot), pl.ds(spot + 1, slots - spot - 1))):
            if cut.size:
                late_copies.append(
                    remote(
                        part.at[peer, cut], landed.at[k, cut], late_sems, 3 * k + n, {"tp": peer}
                    )
                )
        late_copies.append(
            remote(stats.at[peer], lstats.at[k], late_sems, 3 * k + 2, {"tp": peer})
        )
    for copy in late_copies:
        copy.start()

    def over_groups(value):
        return jnp.concatenate(
            [jnp.broadcast_to(value[g : g + 1], (repeat, DH)) for g in range(groups_here)],
            axis=0,
        )

    def merged(i, token, rows_of_stats):
        def entry(stat, place):
            return jnp.sum(jnp.where(column == place, stat, 0.0), axis=1, keepdims=True)

        token = token.astype(jnp.float32)
        keys = over_groups(token[heads_here : heads_here + groups_here])
        values = over_groups(token[heads_here + groups_here :])
        fresh = jnp.sum(token[:heads_here] * keys, axis=-1, keepdims=True) * scaling
        peaks = [entry(stat, i) for stat in rows_of_stats]
        top = fresh
        for peak in peaks:
            top = jnp.maximum(top, peak)
        weight = jnp.exp(fresh - top)
        total = weight
        mixed = weight.astype(jnp.bfloat16).astype(jnp.float32) * values
        for k, stat in enumerate(rows_of_stats):
            scale = jnp.exp(peaks[k] - top)
            block = part[me, i] if k == 0 else landed[k - 1, i]
            total = total + scale * entry(stat, slots + i)
            mixed = mixed + scale * block
        return mixed / total

    for copy in early_copies:
        copy.wait()
    rows_of_stats = [early[me]] + [learly[k] for k in range(parts - 1)]
    row_out[...] = merged(spot, visit[...], rows_of_stats).astype(row_out.dtype)
    row = remote(row_out, row_in, row_sems, 0, {"rep": ahead})
    row.start()

    for copy in late_copies:
        copy.wait()

    @pl.loop(0, slots - 1)
    def _(n):
        i = n + jnp.where(n >= spot, 1, 0)
        rows_of_stats = [stats[me]] + [lstats[k] for k in range(parts - 1)]
        done[i] = merged(i, tokens_ref[i], rows_of_stats)

    done[spot] = jnp.zeros(done.shape[1:], done.dtype)

    @pl.loop(0, slots)
    def _(i):
        index = i - jnp.where(i > leaving, 1, 0)
        place = index + jnp.where(index >= spot, 1, 0)
        ordered[i] = done[jnp.where(i == leaving, spot, place)]

    flat = jnp.concatenate([ordered[:, h, :] for h in range(heads_here)], axis=1)
    if extra:

        @pl.when(gets_paired)
        def _():
            for copy in shared_out:
                copy.wait_recv()
            for copy in posts:
                copy.start()

    row.wait()
    arrived = row_in[...].astype(jnp.float32)
    arrived = jnp.concatenate([arrived[h : h + 1] for h in range(heads_here)], axis=1)
    taken_row = lax.broadcasted_iota(jnp.int32, flat.shape, 0) == leaving
    out_ref[...] = jnp.where(taken_row, arrived, flat).astype(out_ref.dtype)
    if not extra:
        for copy in plain:
            copy.wait()
        return

    @pl.when(sends_paired)
    def _():
        for copy in opening + shared_out + closing:
            copy.wait_send()

    @pl.when(gets_paired)
    def _():
        for copy in opening + closing:
            copy.wait_recv()
        for copy in posts:
            copy.wait()

    @pl.when(jnp.logical_not(sends_paired))
    def _():
        for copy in plain:
            copy.wait_send()

    @pl.when(jnp.logical_not(gets_paired))
    def _():
        for copy in plain:
            copy.wait_recv()


def served(serial, distance, room, lengths, mig_slot, table, queries, keys, values, key_pool, value_pool):
    slots, pages = table.shape
    rows, width = key_pool.shape[1:]
    parts = lax.axis_size("tp")
    heads_here = H // parts
    heads_all = heads_here + 2 * keys.shape[1] // DH
    others = parts - 1
    dtype = queries.dtype
    moved = (pages, rows, width)
    part = (slots, heads_here, DH)
    cuts = 2 if key_pool.shape[0] % 2 == 0 else 1
    extra = pages - room if paired_sources(lax.axis_size("rep"), distance) else 0
    guests = (max(extra, 1), rows, width)
    return pl.pallas_call(
        functools.partial(serve_kernel, distance, room),
        out_shape=[
            jax.ShapeDtypeStruct(queries.shape, dtype),
            jax.ShapeDtypeStruct(moved, dtype),
            jax.ShapeDtypeStruct(moved, dtype),
        ],
        in_specs=[pl.BlockSpec(memory_space=pltpu.HBM)] * 8,
        out_specs=[pl.BlockSpec(memory_space=pltpu.VMEM)] * 3,
        scratch_shapes=[
            pltpu.SMEM(lengths.shape, lengths.dtype),
            pltpu.SMEM(mig_slot.shape, mig_slot.dtype),
            pltpu.SMEM(table.shape, table.dtype),
            pltpu.VMEM(queries.shape, dtype),
            pltpu.VMEM(keys.shape, dtype),
            pltpu.VMEM(values.shape, dtype),
            pltpu.VMEM(key_pool.shape, dtype),
            pltpu.VMEM(key_pool.shape, dtype),
            pltpu.VMEM(moved, dtype),
            pltpu.VMEM(moved, dtype),
            pltpu.VMEM(guests, dtype),
            pltpu.VMEM(guests, dtype),
            pltpu.VMEM((slots, heads_all, DH), jnp.float32),
            pltpu.VMEM(part, dtype),
            pltpu.VMEM((slots, heads_all, DH), dtype),
            pltpu.VMEM((parts,) + part, dtype),
            pltpu.VMEM((heads_all, DH), dtype),
            pltpu.VMEM((parts,) + part, jnp.float32),
            pltpu.VMEM((parts, heads_here, DH), jnp.float32),
            pltpu.VMEM((parts, heads_here, DH), jnp.float32),
            pltpu.VMEM((others,) + part, jnp.float32),
            pltpu.VMEM((others, heads_here, DH), jnp.float32),
            pltpu.VMEM((others, heads_here, DH), jnp.float32),
            pltpu.VMEM((heads_here, DH), dtype),
            pltpu.VMEM((heads_here, DH), dtype),
            pltpu.VMEM(part, jnp.float32),
            pltpu.VMEM(part, jnp.float32),
            pltpu.SemaphoreType.DMA((6,)),
            pltpu.SemaphoreType.DMA((2, cuts)),
            pltpu.SemaphoreType.DMA((2, 10)),
            pltpu.SemaphoreType.DMA((2, max(2 * extra, 1))),
            pltpu.SemaphoreType.DMA((2, 1)),
            pltpu.SemaphoreType.DMA((2, 2 * others)),
            pltpu.SemaphoreType.DMA((2, others)),
            pltpu.SemaphoreType.DMA((2, 2 * others)),
            pltpu.SemaphoreType.DMA((2, 3 * others)),
            pltpu.SemaphoreType.DMA((2, 1)),
        ],
        compiler_params=pltpu.CompilerParams(
            collective_id=2 + serial, has_side_effects=True, vmem_limit_bytes=32 << 20
        ),
        cost_estimate=pl.CostEstimate(
            flops=4 * H * slots * pages * rows * width,
            bytes_accessed=4 * math.prod(key_pool.shape),
            transcendentals=0,
        ),
    )(lengths, mig_slot, table, queries, keys, values, key_pool, value_pool)


def settle_kernel(
    live_ref,
    result_ref,
    key_ref,
    value_ref,
    out_ref,
    kout_ref,
    vout_ref,
    blank,
    result_sem,
    page_sems,
):
    pages = key_ref.shape[0]
    live = live_ref[0]
    lanes = ((key_ref, kout_ref), (value_ref, vout_ref))
    result = pltpu.make_async_copy(result_ref, out_ref, result_sem)
    result.start()
    blank[...] = jnp.zeros_like(blank)
    for j in range(pages):
        for n, (origin, target) in enumerate(lanes):
            spot = target.at[j]
            pl.when(j < live)(pltpu.make_async_copy(origin.at[j], spot, page_sems.at[n]).start)
            pl.when(j >= live)(pltpu.make_async_copy(blank, spot, page_sems.at[n]).start)
    for n, (origin, target) in enumerate(lanes):
        pltpu.make_async_copy(origin, target, page_sems.at[n]).wait()
    result.wait()


def settled(live, *arrays):
    rows, width = arrays[1].shape[1:]
    return pl.pallas_call(
        settle_kernel,
        out_shape=[jax.ShapeDtypeStruct(a.shape, a.dtype) for a in arrays],
        in_specs=[pl.BlockSpec(memory_space=pltpu.SMEM)]
        + [pl.BlockSpec(memory_space=pltpu.VMEM)] * 3,
        out_specs=[pl.BlockSpec(memory_space=pltpu.HBM)] * 3,
        scratch_shapes=[
            pltpu.VMEM((rows, width), arrays[1].dtype),
            pltpu.SemaphoreType.DMA,
            pltpu.SemaphoreType.DMA((2,)),
        ],
        compiler_params=pltpu.CompilerParams(vmem_limit_bytes=8 << 20),
    )(live, *arrays)


def branch_plans(replicas, pages):
    return [
        [(distance, room) for room in room_choices(replicas, distance, pages)]
        for distance in range(1, replicas)
    ]


def choose_kernel(page_len, pages, len_ref, mig_ref, dst_ref, out_ref, live_ref):
    replicas = mig_ref.shape[0]
    slots = len_ref.shape[0] // replicas

    def need(source):
        length = len_ref[source * slots + mig_ref[source]]
        return lax.div(length + (page_len - 1), page_len)

    needs = [need(source) for source in range(replicas)]
    distance = dst_ref[0]
    index, base = jnp.int32(0), 0
    for step, plans in enumerate(branch_plans(replicas, pages), start=1):
        place = jnp.int32(base)
        if len(plans) > 1:
            worst = jnp.int32(0)
            members = paired_sources(replicas, step)
            for source in members[::2]:
                worst = jnp.maximum(worst, needs[source] + needs[source + 1])
            for source in [] if members else passing(replicas, step):
                worst = jnp.maximum(worst, 2 * needs[source])
            for _, room in plans[:-1]:
                place = place + jnp.where(worst > 2 * room, 1, 0)
        index = jnp.where(distance == step, place, index)
        base += len(plans)
    out_ref[0] = index
    live_ref[0] = need(lax.rem(lax.axis_index("rep") + replicas - distance, replicas))


def chosen(page_len, pages, lengths, mig_slot, mig_dst):
    return pl.pallas_call(
        functools.partial(choose_kernel, page_len, pages),
        out_shape=[pltpu.SMEM((1,), jnp.int32)] * 2,
        in_specs=[pl.BlockSpec(memory_space=pltpu.SMEM)] * 3,
        out_specs=[pl.BlockSpec(memory_space=pltpu.SMEM)] * 2,
    )(lengths, mig_slot, mig_dst)


def swift_body(
    queries, new_keys, new_values, key_pool, value_pool, lengths, page_table, mig_slot, mig_dst
):
    replicas = lax.axis_size("rep")
    pages = page_table.shape[1]
    page_len = key_pool.shape[1] * lax.axis_size("tp")
    plans = [plan for group in branch_plans(replicas, pages) for plan in group]
    index, live = chosen(page_len, pages, lengths, mig_slot, mig_dst)
    results = lax.switch(
        index[0],
        [functools.partial(served, n, *plan) for n, plan in enumerate(plans)],
        lengths,
        mig_slot,
        page_table,
        queries,
        new_keys,
        new_values,
        key_pool,
        value_pool,
    )
    return settled(live, *results)


def solution(mesh):
    placed = (
        P("rep", "tp"),
        P("rep", "tp"),
        P("rep", "tp"),
        P("rep", "tp", None),
        P("rep", "tp", None),
        P(),
        P("rep", None),
        P(),
        P(),
    )
    swift = KVH % mesh.shape["tp"] == 0
    return jax.shard_map(
        swift_body if swift else body,
        mesh=mesh,
        in_specs=placed,
        out_specs=(P("rep", "tp"), P("rep", "tp", None), P("rep", "tp", None)),
        check_vma=False,
    )
```

```python
import functools
import math


import jax
import jax.numpy as jnp
from jax import lax
from jax.experimental import pallas as pl
from jax.experimental.pallas import tpu as pltpu
from jax.sharding import PartitionSpec as P

H = 64
KVH = 8
DH = 128
LOW = -1e30


def route_by(count, distance):
    return [(i, (i + distance) % count) for i in range(count)]


def pick_kernel(
    table_ref, mig_ref, q_ref, nk_ref, nv_ref, key_ref, value_ref, row_ref, kout_ref, vout_ref, sems
):
    pages = kout_ref.shape[0]
    leaving = mig_ref[lax.axis_index("rep")]

    @pl.loop(0, pages)
    def _(j):
        page = jnp.maximum(table_ref[leaving, j], 0)
        pltpu.make_async_copy(key_ref.at[page], kout_ref.at[j], sems.at[0]).start()
        pltpu.make_async_copy(value_ref.at[page], vout_ref.at[j], sems.at[1]).start()

    at = 0
    for ref in (q_ref, nk_ref, nv_ref):
        width = ref.shape[1]
        slot = lax.broadcasted_iota(jnp.int32, ref.shape, 0)
        chosen = jnp.where(slot == leaving, ref[...].astype(jnp.float32), 0.0)
        row = jnp.sum(chosen, axis=0, keepdims=True)
        row_ref[:, at : at + width] = row.astype(jnp.bfloat16)
        at += width
    pltpu.make_async_copy(key_ref.at[pl.ds(0, pages)], kout_ref, sems.at[0]).wait()
    pltpu.make_async_copy(value_ref.at[pl.ds(0, pages)], vout_ref, sems.at[1]).wait()

    @pl.loop(0, pages)
    def _(j):
        @pl.when(table_ref[leaving, j] < 0)
        def _():
            kout_ref[j] = jnp.zeros(kout_ref.shape[1:], kout_ref.dtype)
            vout_ref[j] = jnp.zeros(vout_ref.shape[1:], vout_ref.dtype)


def picked(table, mig_slot, queries, new_keys, new_values, key_pool, value_pool):
    shape = (table.shape[1],) + key_pool.shape[1:]
    width = queries.shape[1] + 2 * new_keys.shape[1]
    return pl.pallas_call(
        pick_kernel,
        out_shape=[
            jax.ShapeDtypeStruct((1, width), jnp.bfloat16),
            jax.ShapeDtypeStruct(shape, key_pool.dtype),
            jax.ShapeDtypeStruct(shape, key_pool.dtype),
        ],
        in_specs=[pl.BlockSpec(memory_space=pltpu.SMEM)] * 2
        + [pl.BlockSpec(memory_space=pltpu.VMEM)] * 3
        + [pl.BlockSpec(memory_space=pl.ANY)] * 2,
        out_specs=[pl.BlockSpec(memory_space=pltpu.VMEM)] * 3,
        scratch_shapes=[pltpu.SemaphoreType.DMA((2,))],
        compiler_params=pltpu.CompilerParams(vmem_limit_bytes=8 << 20),
        cost_estimate=pl.CostEstimate(
            flops=0, bytes_accessed=8 * math.prod(shape), transcendentals=0
        ),
    )(table, mig_slot, queries, new_keys, new_values, key_pool, value_pool)


def greet(parts):
    me = lax.axis_index("tp")
    barrier = pltpu.get_barrier_semaphore()
    for k in range(1, parts):
        pl.semaphore_signal(
            barrier,
            inc=1,
            device_id={"tp": lax.rem(me + k, parts)},
            device_id_type=pl.DeviceIdType.MESH,
        )
    pl.semaphore_wait(barrier, parts - 1)
    return me


def share_kernel(mig_ref, back_ref, tokens_ref, all_ref, mine_ref, own, send_sems, recv_sems):
    parts, slots, heads_here, _ = all_ref.shape
    chunks = tokens_ref.shape[1]
    leaving = mig_ref[lax.axis_index("rep")]
    back = back_ref[...].astype(jnp.float32)
    row = jnp.concatenate([back[:, h * DH : (h + 1) * DH] for h in range(chunks)], axis=0)
    for i in range(slots):
        value = jnp.where(leaving == i, row, tokens_ref[i].astype(jnp.float32))
        value = value.astype(jnp.bfloat16)
        mine_ref[i] = value
        own[i] = value[:heads_here]
    me = greet(parts)
    copies = []
    for k in range(1, parts):
        copy = pltpu.make_async_remote_copy(
            src_ref=own,
            dst_ref=all_ref.at[me],
            send_sem=send_sems.at[k - 1],
            recv_sem=recv_sems.at[k - 1],
            device_id={"tp": lax.rem(me + k, parts)},
            device_id_type=pl.DeviceIdType.MESH,
        )
        copy.start()
        copies.append(copy)
    all_ref[me] = own[...]
    for copy in copies:
        copy.wait()


def shared(mig_slot, back, tokens, heads_here, parts):
    slots = tokens.shape[0]
    return pl.pallas_call(
        share_kernel,
        out_shape=[
            jax.ShapeDtypeStruct((parts, slots, heads_here, DH), jnp.bfloat16),
            jax.ShapeDtypeStruct(tokens.shape, jnp.bfloat16),
        ],
        in_specs=[pl.BlockSpec(memory_space=pltpu.SMEM)]
        + [pl.BlockSpec(memory_space=pltpu.VMEM)] * 2,
        out_specs=[pl.BlockSpec(memory_space=pltpu.VMEM)] * 2,
        scratch_shapes=[
            pltpu.VMEM((slots, heads_here, DH), jnp.bfloat16),
            pltpu.SemaphoreType.DMA((parts - 1,)),
            pltpu.SemaphoreType.DMA((parts - 1,)),
        ],
        compiler_params=pltpu.CompilerParams(
            collective_id=0, has_side_effects=True, vmem_limit_bytes=8 << 20
        ),
        cost_estimate=pl.CostEstimate(flops=0, bytes_accessed=8 << 20, transcendentals=0),
    )(mig_slot, back, tokens)


def flat_rows(block):
    pages, rows, width = block.shape
    if rows % 16 == 0:
        return block.reshape(pages * rows, width)
    return block.astype(jnp.float32).reshape(pages * rows, width).astype(block.dtype)


def attend_kernel(
    table_ref,
    len_ref,
    start_ref,
    q_ref,
    key_ref,
    value_ref,
    out_ref,
    kbuf,
    vbuf,
    stats_ref,
    ksem,
    vsem,
):
    slots, pages, rows, width = kbuf.shape
    parts, heads_here = q_ref.shape[0], q_ref.shape[2]
    group = H // KVH
    page_len = rows * parts
    scaling = 1.0 / math.sqrt(DH)
    steps = 3 if pages % 3 == 0 else 1
    step_pages = pages // steps

    def live_pages(i):
        return lax.div(len_ref[i] + (page_len - 1), page_len)

    def key_copy(i, j):
        page = jnp.maximum(table_ref[i, j], 0)
        return pltpu.make_async_copy(key_ref.at[page], kbuf.at[i, j], ksem.at[i, j])

    def value_copy(i, j):
        page = jnp.maximum(table_ref[i, j], 0)
        return pltpu.make_async_copy(value_ref.at[page], vbuf.at[i, j], vsem.at[i, j])

    @pl.loop(0, slots)
    def _(i):
        @pl.loop(0, live_pages(i))
        def _(j):
            key_copy(i, j).start()
            value_copy(i, j).start()

    head = lax.broadcasted_iota(jnp.int32, (H, DH), 0) // group
    column = lax.broadcasted_iota(jnp.int32, (H, DH), 1)
    stats_ref[...] = jnp.zeros_like(stats_ref)

    def attend(i, used):
        tokens = used * rows
        lane = lax.broadcasted_iota(jnp.int32, (H, tokens), 1)
        position = (lane // rows) * page_len + lane % rows + start_ref[0]
        q = jnp.concatenate([q_ref[t, i].astype(jnp.float32) for t in range(parts)], axis=0)
        spread = jnp.concatenate(
            [jnp.where(head == g, q, 0.0).astype(jnp.bfloat16) for g in range(KVH)], axis=1
        )
        scores = lax.dot_general(
            spread,
            flat_rows(kbuf[i, 0:used]),
            (((1,), (1,)), ((), ())),
            preferred_element_type=jnp.float32,
        )
        usable = position < len_ref[i]
        masked = jnp.where(usable, scores * scaling, LOW)
        peak = jnp.max(masked, axis=1, keepdims=True)
        weights = jnp.where(usable, jnp.exp(masked - peak), 0.0)
        total = jnp.sum(weights, axis=1, keepdims=True)
        mixed = jnp.dot(
            weights.astype(jnp.bfloat16),
            flat_rows(vbuf[i, 0:used]),
            preferred_element_type=jnp.float32,
        )
        own = jnp.concatenate(
            [
                mixed[g * group : (g + 1) * group, g * DH : (g + 1) * DH]
                for g in range(KVH)
            ],
            axis=0,
        )
        for t in range(parts):
            out_ref[t, i] = own[t * heads_here : (t + 1) * heads_here]
        stats = jnp.where(column == i, peak, stats_ref[...])
        stats_ref[...] = jnp.where(column == i + slots, total, stats)

    @pl.loop(0, slots)
    def _(i):
        live = live_pages(i)
        needed = lax.div(live + (step_pages - 1), step_pages)

        @pl.loop(live, needed * step_pages)
        def _(j):
            vbuf[i, j] = jnp.zeros((rows, width), vbuf.dtype)

        @pl.loop(0, live)
        def _(j):
            key_copy(i, j).wait()
            value_copy(i, j).wait()

        for step in range(1, steps + 1):

            @pl.when(needed == step)
            def _():
                attend(i, step * step_pages)

    for t in range(parts):
        out_ref[t, slots] = stats_ref[t * heads_here : (t + 1) * heads_here]


def attended_parts(table, lens, start, q, key_pool, value_pool, parts):
    slots, pages = table.shape
    rows, width = key_pool.shape[1:]
    buffer = (slots, pages, rows, width)
    return pl.pallas_call(
        attend_kernel,
        out_shape=jax.ShapeDtypeStruct((parts, slots + 1, H // parts, DH), jnp.float32),
        in_specs=[pl.BlockSpec(memory_space=pltpu.SMEM)] * 3
        + [pl.BlockSpec(memory_space=pltpu.VMEM)]
        + [pl.BlockSpec(memory_space=pl.ANY)] * 2,
        out_specs=pl.BlockSpec(memory_space=pltpu.VMEM),
        scratch_shapes=[
            pltpu.VMEM(buffer, key_pool.dtype),
            pltpu.VMEM(buffer, value_pool.dtype),
            pltpu.VMEM((H, DH), jnp.float32),
            pltpu.SemaphoreType.DMA((slots, pages)),
            pltpu.SemaphoreType.DMA((slots, pages)),
        ],
        compiler_params=pltpu.CompilerParams(vmem_limit_bytes=24 << 20),
        cost_estimate=pl.CostEstimate(
            flops=4 * H * pages * rows * width * slots,
            bytes_accessed=4 * math.prod(buffer),
            transcendentals=0,
        ),
    )(table, lens, start, q, key_pool, value_pool)


def finish_kernel(
    mig_ref,
    part_ref,
    mine_ref,
    tk_ref,
    tv_ref,
    out_ref,
    leaver_ref,
    flat,
    landed,
    send_sems,
    recv_sems,
):
    parts, _, heads_here, _ = part_ref.shape
    slots = mine_ref.shape[0]
    repeat = heads_here // tk_ref.shape[1]
    leaving = mig_ref[lax.axis_index("rep")]
    scaling = 1.0 / math.sqrt(DH)
    me = greet(parts)
    copies = []
    for k in range(1, parts):
        peer = lax.rem(me + k, parts)
        copy = pltpu.make_async_remote_copy(
            src_ref=part_ref.at[peer],
            dst_ref=landed.at[k - 1],
            send_sem=send_sems.at[k - 1],
            recv_sem=recv_sems.at[k - 1],
            device_id={"tp": peer},
            device_id_type=pl.DeviceIdType.MESH,
        )
        copy.start()
        copies.append(copy)

    def spread(ref, i):
        value = ref[i].astype(jnp.float32)
        return jnp.concatenate(
            [
                jnp.broadcast_to(value[g : g + 1], (repeat, DH))
                for g in range(value.shape[0])
            ],
            axis=0,
        )

    fresh, values = [], []
    for i in range(slots):
        q = mine_ref[i].astype(jnp.float32)[:heads_here]
        fresh.append(jnp.sum(q * spread(tk_ref, i), axis=-1, keepdims=True) * scaling)
        values.append(spread(tv_ref, i))
    for copy in copies:
        copy.wait()
    stats = [part_ref[me, slots]] + [landed[k, slots] for k in range(parts - 1)]
    leaver = jnp.zeros((heads_here, DH), jnp.float32)
    for i in range(slots):
        top = fresh[i]
        for stat in stats:
            top = jnp.maximum(top, stat[:, i : i + 1])
        weight = jnp.exp(fresh[i] - top)
        total = weight
        mixed = weight.astype(jnp.bfloat16).astype(jnp.float32) * values[i]
        for k, stat in enumerate(stats):
            scale = jnp.exp(stat[:, i : i + 1] - top)
            block = part_ref[me, i] if k == 0 else landed[k - 1, i]
            total = total + scale * stat[:, slots + i : slots + i + 1]
            mixed = mixed + scale * block
        result = mixed / total
        leaver = jnp.where(leaving == i, result, leaver)
        for h in range(heads_here):
            flat[i : i + 1, h * DH : (h + 1) * DH] = result[h : h + 1]
    out_ref[...] = flat[...].astype(out_ref.dtype)
    row = jnp.concatenate([leaver[h : h + 1] for h in range(heads_here)], axis=1)
    leaver_ref[...] = row.astype(leaver_ref.dtype)


def finished(mig_slot, partials, mine, token_keys, token_values):
    parts, _, heads_here, _ = partials.shape
    slots = mine.shape[0]
    return pl.pallas_call(
        finish_kernel,
        out_shape=[
            jax.ShapeDtypeStruct((slots, heads_here * DH), jnp.bfloat16),
            jax.ShapeDtypeStruct((1, heads_here * DH), jnp.bfloat16),
        ],
        in_specs=[pl.BlockSpec(memory_space=pltpu.SMEM)]
        + [pl.BlockSpec(memory_space=pltpu.VMEM)] * 4,
        out_specs=[pl.BlockSpec(memory_space=pltpu.VMEM)] * 2,
        scratch_shapes=[
            pltpu.VMEM((slots, heads_here * DH), jnp.float32),
            pltpu.VMEM((parts - 1,) + partials.shape[1:], jnp.float32),
            pltpu.SemaphoreType.DMA((parts - 1,)),
            pltpu.SemaphoreType.DMA((parts - 1,)),
        ],
        compiler_params=pltpu.CompilerParams(
            collective_id=1, has_side_effects=True, vmem_limit_bytes=8 << 20
        ),
        cost_estimate=pl.CostEstimate(flops=0, bytes_accessed=8 << 20, transcendentals=0),
    )(mig_slot, partials, mine, token_keys, token_values)


def place_kernel(
    mig_ref, result_ref, row_ref, key_ref, value_ref, out_ref, kout_ref, vout_ref, kbuf, vbuf, sems
):
    pages = kbuf.shape[0]
    lanes = ((key_ref, kbuf, kout_ref), (value_ref, vbuf, vout_ref))
    span = 3 if pages % 3 == 0 else 1
    cuts = [pl.ds(j, span) for j in range(0, pages, span)]
    pairs = [(n, c) for c in range(len(cuts)) for n in range(2)]
    for n, c in pairs:
        source, buf, _ = lanes[n]
        pltpu.make_async_copy(source.at[cuts[c]], buf.at[cuts[c]], sems.at[n, c]).start()
    leaving = mig_ref[lax.axis_index("rep")]
    slot = lax.broadcasted_iota(jnp.int32, result_ref.shape, 0)
    row = row_ref[...].astype(jnp.float32)
    result = result_ref[...].astype(jnp.float32)
    out_ref[...] = jnp.where(slot == leaving, row, result).astype(out_ref.dtype)
    for n, c in pairs:
        source, buf, sink = lanes[n]
        pltpu.make_async_copy(source.at[cuts[c]], buf.at[cuts[c]], sems.at[n, c]).wait()
        pltpu.make_async_copy(buf.at[cuts[c]], sink.at[cuts[c]], sems.at[n, c]).start()
    for n, c in pairs:
        _, buf, sink = lanes[n]
        pltpu.make_async_copy(buf.at[cuts[c]], sink.at[cuts[c]], sems.at[n, c]).wait()


def placed_results(mig_slot, result, row, moved_keys, moved_values):
    moved = jax.ShapeDtypeStruct(moved_keys.shape, moved_keys.dtype)
    return pl.pallas_call(
        place_kernel,
        out_shape=[jax.ShapeDtypeStruct(result.shape, result.dtype), moved, moved],
        in_specs=[pl.BlockSpec(memory_space=pltpu.SMEM)]
        + [pl.BlockSpec(memory_space=pltpu.VMEM)] * 2
        + [pl.BlockSpec(memory_space=pl.ANY)] * 2,
        out_specs=[pl.BlockSpec(memory_space=pltpu.VMEM)]
        + [pl.BlockSpec(memory_space=pl.ANY)] * 2,
        scratch_shapes=[
            pltpu.VMEM(moved.shape, moved.dtype),
            pltpu.VMEM(moved.shape, moved.dtype),
            pltpu.SemaphoreType.DMA((2, moved.shape[0])),
        ],
        compiler_params=pltpu.CompilerParams(vmem_limit_bytes=8 << 20),
    )(mig_slot, result, row, moved_keys, moved_values)


def token_rows(fresh, parts, part_index):
    slots, width = fresh.shape
    heads_here = H // parts
    if width % DH == 0:
        return fresh.reshape(slots, width // DH, DH)
    every = lax.all_gather(fresh, "tp", axis=1, tiled=True).reshape(slots, KVH, DH)
    every = jnp.repeat(every, H // KVH, axis=1)
    return lax.dynamic_slice_in_dim(every, part_index * heads_here, heads_here, 1)


def body(
    queries, new_keys, new_values, key_pool, value_pool, lengths, page_table, mig_slot, mig_dst
):
    replicas = lax.axis_size("rep")
    parts = lax.axis_size("tp")
    here_rep = lax.axis_index("rep")
    part_index = lax.axis_index("tp")
    slots, _ = queries.shape
    k_width = new_keys.shape[1]
    heads_here = H // parts
    offset = mig_dst[0]
    start = (part_index * key_pool.shape[1]).reshape(1)
    visitor, keys_out, values_out = picked(
        page_table, mig_slot, queries, new_keys, new_values, key_pool, value_pool
    )

    def branch(distance):
        def run(visitor, keys_out, values_out):
            back = lax.ppermute(visitor, "rep", route_by(replicas, -distance))
            moved_keys = lax.ppermute(keys_out, "rep", route_by(replicas, distance))
            moved_values = lax.ppermute(values_out, "rep", route_by(replicas, distance))
            own_len = lax.dynamic_slice_in_dim(lengths, here_rep * slots, slots)
            tokens = jnp.concatenate([queries, new_keys, new_values], axis=1)
            tokens = tokens.reshape(slots, -1, DH)
            q_all, mine = shared(mig_slot, back, tokens, heads_here, parts)
            flat = mine[:, heads_here:].reshape(slots, 2 * k_width)
            token_keys = token_rows(flat[:, :k_width], parts, part_index)
            token_values = token_rows(flat[:, k_width:], parts, part_index)
            partials = attended_parts(
                page_table, own_len, start, q_all, key_pool, value_pool, parts
            )
            result, leaver = finished(mig_slot, partials, mine, token_keys, token_values)
            arrived = lax.ppermute(leaver, "rep", route_by(replicas, distance))
            return result, arrived, moved_keys, moved_values

        return run

    result, arrived, moved_keys, moved_values = lax.switch(
        offset - 1,
        [branch(distance) for distance in range(1, replicas)],
        visitor,
        keys_out,
        values_out,
    )
    return placed_results(mig_slot, result, arrived, moved_keys, moved_values)


def leaver_place(slots):
    return min(3, slots - 1)


def crossing(replicas, distance):
    cuts = {}
    for source in range(replicas):
        start, end = source // 2, (source + distance) % replicas // 2
        for chip in range(min(start, end), max(start, end)):
            cuts.setdefault((chip, end > start), []).append(source)
    return cuts


def paired_sources(replicas, distance):
    cuts = crossing(replicas, distance).values()
    most = max(map(len, cuts))
    busiest = [flows for flows in cuts if len(flows) == most]
    return [
        s for s in range(replicas) if any(s in flows and s ^ 1 in flows for flows in busiest)
    ]


def lone_sources(replicas, distance):
    cuts = crossing(replicas, distance).values()
    most = max(map(len, cuts))
    members = paired_sources(replicas, distance)
    return [
        s
        for s in range(replicas)
        if s not in members and any(s in flows and len(flows) == most for flows in cuts)
    ]


def branch_plans(replicas, pages):
    plans = []
    for distance in range(1, replicas):
        rooms, singles = [pages], [pages]
        if replicas % 2 == 0:
            low, mid = pages * 2 // 3, pages * 5 // 6
            paired = paired_sources(replicas, distance)
            if paired:
                rooms = [low, mid, pages]
            if 2 * distance == replicas:
                rooms.append(pages * 3 // 4)
            if lone_sources(replicas, distance):
                singles = [low, pages] if paired else [low, mid, pages]
        plans.append((distance, sorted(set(rooms)), sorted(set(singles))))
    return plans


def among(index, members):
    found = index < 0
    for member in members:
        found = found | (index == member)
    return found


def slot_at(place, leaving, spot):
    index = place - jnp.where(place > spot, 1, 0)
    other = index + jnp.where(index >= leaving, 1, 0)
    return jnp.where(place == spot, leaving, other)


def serve_kernel(
    distance,
    room,
    single,
    len_hbm,
    mig_hbm,
    table_hbm,
    queries_hbm,
    keys_hbm,
    values_hbm,
    key_hbm,
    value_hbm,
    out_ref,
    kout_ref,
    vout_ref,
    len_ref,
    mig_ref,
    table_ref,
    queries_ref,
    keys_ref,
    values_ref,
    kpool,
    vpool,
    ksend,
    vsend,
    kguest,
    vguest,
    loose,
    q_ref,
    tokens_ref,
    q_all,
    q_visit,
    visit,
    part,
    early,
    landed,
    learly,
    row_out,
    row_in,
    done,
    ordered,
    small_sems,
    pool_sems,
    bulk_sems,
    post_sems,
    visit_sems,
    share_sems,
    relay_sems,
    early_sems,
    late_sems,
    row_sems,
):
    pages, rows, _ = kout_ref.shape
    slots, heads_here = q_ref.shape[:2]
    groups_here = (tokens_ref.shape[1] - heads_here) // 2
    replicas, parts = lax.axis_size("rep"), lax.axis_size("tp")
    rep, me = lax.axis_index("rep"), lax.axis_index("tp")
    spot = leaver_place(slots)
    group = H // KVH
    repeat = heads_here // groups_here
    page_len = rows * parts
    scaling = 1.0 / math.sqrt(DH)
    ahead = lax.rem(rep + distance, replicas)
    behind = lax.rem(rep + replicas - distance, replicas)
    peers = [lax.rem(me + k, parts) for k in range(1, parts)]
    mesh_id = pl.DeviceIdType.MESH

    extra = pages - room
    members = paired_sources(replicas, distance) if extra else []
    lone = lone_sources(replicas, distance) if single < pages else []
    rest = [s for s in range(replicas) if s not in members and s not in lone]

    def when(index, group):
        if len(group) == replicas:
            return lambda run: run()
        return pl.when(among(index, group)) if group else lambda run: None

    partner = rep + 1 - 2 * lax.rem(rep, 2)
    mate = lax.rem(behind + 1 - 2 * lax.rem(behind, 2) + distance, replicas)

    barrier = pltpu.get_barrier_semaphore()

    def greet_rep(other):
        pl.semaphore_signal(barrier, inc=1, device_id={"rep": other}, device_id_type=mesh_id)

    for other in (ahead, behind):
        greet_rep(other)
    for peer in peers:
        pl.semaphore_signal(barrier, inc=1, device_id={"tp": peer}, device_id_type=mesh_id)
    if extra:
        greet_rep(partner)
        if distance % 2:
            greet_rep(mate)

    smalls = [
        pltpu.make_async_copy(source, target, small_sems.at[n])
        for n, (source, target) in enumerate(
            (
                (table_hbm, table_ref),
                (mig_hbm, mig_ref),
                (len_hbm, len_ref),
                (queries_hbm, queries_ref),
                (keys_hbm, keys_ref),
                (values_hbm, values_ref),
            )
        )
    ]
    for copy in smalls:
        copy.start()
    loads = []
    cuts = pool_sems.shape[1]
    step = kpool.shape[0] // cuts
    for n, (source, target) in enumerate(((key_hbm, kpool), (value_hbm, vpool))):
        for c in range(cuts):
            cut = pl.ds(c * step, step)
            loads.append(
                pltpu.make_async_copy(source.at[cut], target.at[cut], pool_sems.at[n, c])
            )
    for copy in loads[:cuts]:
        copy.start()

    for copy in smalls:
        copy.wait()
    leaving = mig_ref[rep]
    row_of = 0
    for ref in (queries_ref, keys_ref, values_ref):
        whole = ref[...].astype(jnp.float32)
        for h in range(ref.shape[1] // DH):
            loose[:, row_of, :] = whole[:, h * DH : (h + 1) * DH]
            row_of += 1
    for i in range(slots):
        token = loose[slot_at(i, leaving, spot)].astype(q_ref.dtype)
        tokens_ref[i] = token
        q_ref[i] = token[:heads_here]

    def fill(target, pool):
        @pl.loop(0, pages)
        def _(j):
            target[j] = pool[jnp.maximum(table_ref[leaving, j], 0)]

    for copy in loads[:cuts]:
        copy.wait()
    for copy in loads[cuts:]:
        copy.start()
    fill(ksend, kpool)
    pl.semaphore_wait(barrier, parts + 1 + (1 + distance % 2 if extra else 0))

    def remote(source, target, sems, k, device):
        return pltpu.make_async_remote_copy(
            src_ref=source,
            dst_ref=target,
            send_sem=sems.at[0, k],
            recv_sem=sems.at[1, k],
            device_id=device,
            device_id_type=mesh_id,
        )

    visitor = remote(tokens_ref.at[spot], visit, visit_sems, 0, {"rep": behind})
    visitor.start()
    shares = [
        remote(q_ref, q_all.at[me], share_sems, k, {"tp": peer}) for k, peer in enumerate(peers)
    ]

    main = room - extra
    first = min(2, main)
    to_ahead, to_partner, to_mate = {"rep": ahead}, {"rep": partner}, {"rep": mate}
    lanes = ((ksend, kguest, kout_ref), (vsend, vguest, vout_ref))

    def cut_copy(n, kind, low, high):
        source, _, target = lanes[n]
        cut = pl.ds(low, high - low)
        return remote(source.at[cut], target.at[cut], bulk_sems, 2 * kind + n, to_ahead)

    plain = [cut_copy(n, 0, 0, pages) for n in range(2)] if rest else []
    short = [cut_copy(n, 4, 0, single) for n in range(2)] if lone else []
    opening, shared_out, closing, swaps, posts = [], [], [], [], []
    if extra:
        if first:
            opening = [cut_copy(n, 1, 0, first) for n in range(2)]
        shared_out = [cut_copy(n, 2, main, room) for n in range(2)]
        if main > first:
            closing = [cut_copy(n, 3, first, main) for n in range(2)]
        for n, (source, guest, target) in enumerate(lanes):
            swaps.append(
                remote(source.at[pl.ds(room, extra)], guest, bulk_sems, 10 + n, to_partner)
            )
            for i in range(extra):
                posts.append(
                    remote(
                        target.at[room - 1 - i],
                        target.at[room + i],
                        post_sems,
                        n * extra + i,
                        to_mate,
                    )
                )

    def send(n):
        @when(rep, members)
        def _():
            swaps[n].start()
            if opening:
                opening[n].start()

        when(rep, lone)(lambda: short[n].start())
        when(rep, rest)(lambda: plain[n].start())

    send(0)
    for copy in shares:
        copy.start()
    q_all[me] = q_ref[...]
    for copy in loads[cuts:]:
        copy.wait()
    fill(vsend, vpool)
    send(1)

    visitor.wait()
    relays = [
        remote(visit.at[pl.ds(0, heads_here)], q_visit.at[me], relay_sems, k, {"tp": peer})
        for k, peer in enumerate(peers)
    ]
    for copy in relays:
        copy.start()
    q_visit[me] = visit[0:heads_here]
    for copy in shares:
        copy.wait()

    @when(rep, members)
    def _():
        theirs = len_ref[partner * slots + mig_ref[partner]]
        for n, (source, guest, _) in enumerate(lanes):
            swaps[n].wait()

            @pl.loop(0, extra)
            def _(i):
                spare = room - 1 - i
                guested = theirs > (room + i) * page_len
                source[spare] = jnp.where(guested, guest[i], source[spare])

            shared_out[n].start()
        for copy in closing:
            copy.start()

    head = lax.broadcasted_iota(jnp.int32, (H, DH), 0) // group
    column = lax.broadcasted_iota(jnp.int32, (heads_here, DH), 1)
    lane = lax.broadcasted_iota(jnp.int32, (H, pages * rows), 1)
    position = (lane // rows) * page_len + lane % rows + me * rows
    part[:, slots] = jnp.zeros((parts, heads_here, DH), part.dtype)
    early_copies = [
        remote(early.at[peer], learly.at[k], early_sems, k, {"tp": peer})
        for k, peer in enumerate(peers)
    ]

    @pl.loop(0, slots)
    def _(i):
        @pl.when(i == spot)
        def _():
            for copy in relays:
                copy.wait()
            for t in range(parts):
                q_all[t, spot] = q_visit[t]

        slot = slot_at(i, leaving, spot)
        length = len_ref[rep * slots + slot]

        def cached(pool):
            return jnp.concatenate(
                [pool[jnp.maximum(table_ref[slot, j], 0)] for j in range(pages)], axis=0
            )

        q = jnp.concatenate([q_all[t, i].astype(jnp.float32) for t in range(parts)], axis=0)
        spread = jnp.concatenate(
            [jnp.where(head == g, q, 0.0).astype(jnp.bfloat16) for g in range(KVH)], axis=1
        )
        scores = lax.dot_general(
            spread, cached(kpool), (((1,), (1,)), ((), ())), preferred_element_type=jnp.float32
        )
        usable = position < length
        masked = jnp.where(usable, scores * scaling, LOW)
        peak = jnp.max(masked, axis=1, keepdims=True)
        weights = jnp.where(usable, jnp.exp(masked - peak), 0.0)
        total = jnp.sum(weights, axis=1, keepdims=True)
        mixed = jnp.dot(
            weights.astype(jnp.bfloat16), cached(vpool), preferred_element_type=jnp.float32
        )
        own = jnp.concatenate(
            [mixed[g * group : (g + 1) * group, g * DH : (g + 1) * DH] for g in range(KVH)],
            axis=0,
        )
        for t in range(parts):
            cut = slice(t * heads_here, (t + 1) * heads_here)
            part[t, i] = own[cut]
            kept = jnp.where(column == i, peak[cut], part[t, slots])
            part[t, slots] = jnp.where(column == i + slots, total[cut], kept)

        @pl.when(i == spot)
        def _():
            early[:, 0] = part[:, spot]
            early[:, 1] = part[:, slots]
            for copy in early_copies:
                copy.start()

    late_copies = [
        remote(part.at[peer], landed.at[k], late_sems, k, {"tp": peer})
        for k, peer in enumerate(peers)
    ]
    for copy in late_copies:
        copy.start()

    def over_groups(value):
        return jnp.concatenate(
            [jnp.broadcast_to(value[g : g + 1], (repeat, DH)) for g in range(groups_here)],
            axis=0,
        )

    def merged(i, token, blocks, rows_of_stats):
        def entry(stat, place):
            return jnp.sum(jnp.where(column == place, stat, 0.0), axis=1, keepdims=True)

        token = token.astype(jnp.float32)
        keys = over_groups(token[heads_here : heads_here + groups_here])
        values = over_groups(token[heads_here + groups_here :])
        fresh = jnp.sum(token[:heads_here] * keys, axis=-1, keepdims=True) * scaling
        peaks = [entry(stat, i) for stat in rows_of_stats]
        top = fresh
        for peak in peaks:
            top = jnp.maximum(top, peak)
        weight = jnp.exp(fresh - top)
        total = weight
        mixed = weight.astype(jnp.bfloat16).astype(jnp.float32) * values
        for k, stat in enumerate(rows_of_stats):
            scale = jnp.exp(peaks[k] - top)
            total = total + scale * entry(stat, slots + i)
            mixed = mixed + scale * blocks[k]
        return mixed / total

    for copy in early_copies:
        copy.wait()
    blocks = [early[me, 0]] + [learly[k, 0] for k in range(parts - 1)]
    rows_of_stats = [early[me, 1]] + [learly[k, 1] for k in range(parts - 1)]
    row_out[...] = merged(spot, visit[...], blocks, rows_of_stats).astype(row_out.dtype)
    row = remote(row_out, row_in, row_sems, 0, {"rep": ahead})
    row.start()

    for copy in late_copies:
        copy.wait()

    @pl.loop(0, slots - 1)
    def _(n):
        i = n + jnp.where(n >= spot, 1, 0)
        blocks = [part[me, i]] + [landed[k, i] for k in range(parts - 1)]
        rows_of_stats = [part[me, slots]] + [landed[k, slots] for k in range(parts - 1)]
        done[i] = merged(i, tokens_ref[i], blocks, rows_of_stats)

    done[spot] = jnp.zeros(done.shape[1:], done.dtype)

    @pl.loop(0, slots)
    def _(i):
        index = i - jnp.where(i > leaving, 1, 0)
        place = index + jnp.where(index >= spot, 1, 0)
        ordered[i] = done[jnp.where(i == leaving, spot, place)]

    flat = jnp.concatenate([ordered[:, h, :] for h in range(heads_here)], axis=1)

    @when(behind, members)
    def _():
        for copy in shared_out:
            copy.wait_recv()
        for copy in posts:
            copy.start()

    row.wait()
    arrived = row_in[...].astype(jnp.float32)
    arrived = jnp.concatenate([arrived[h : h + 1] for h in range(heads_here)], axis=1)
    taken_row = lax.broadcasted_iota(jnp.int32, flat.shape, 0) == leaving
    out_ref[...] = jnp.where(taken_row, arrived, flat).astype(out_ref.dtype)

    def settle_all(copies, name):
        for copy in copies:
            getattr(copy, name)()

    sends = ((members, opening + shared_out + closing), (lone, short), (rest, plain))
    gets = ((members, opening + closing), (lone, short), (rest, plain))
    for group, copies in sends:
        when(rep, group)(functools.partial(settle_all, copies, "wait_send"))
    for group, copies in gets:
        when(behind, group)(functools.partial(settle_all, copies, "wait_recv"))
    when(behind, members)(functools.partial(settle_all, posts, "wait"))


def served(serial, distance, room, single, lengths, mig_slot, table, queries, keys, values, key_pool, value_pool):
    slots, pages = table.shape
    rows, width = key_pool.shape[1:]
    parts = lax.axis_size("tp")
    heads_here = H // parts
    heads_all = heads_here + 2 * keys.shape[1] // DH
    others = parts - 1
    dtype = queries.dtype
    moved = (pages, rows, width)
    part = (slots, heads_here, DH)
    cuts = 2 if key_pool.shape[0] % 2 == 0 else 1
    extra = pages - room
    guests = (max(extra, 1), rows, width)
    return pl.pallas_call(
        functools.partial(serve_kernel, distance, room, single),
        out_shape=[
            jax.ShapeDtypeStruct(queries.shape, dtype),
            jax.ShapeDtypeStruct(moved, dtype),
            jax.ShapeDtypeStruct(moved, dtype),
        ],
        in_specs=[pl.BlockSpec(memory_space=pltpu.HBM)] * 8,
        out_specs=[pl.BlockSpec(memory_space=pltpu.VMEM)] * 3,
        scratch_shapes=[
            pltpu.SMEM(lengths.shape, lengths.dtype),
            pltpu.SMEM(mig_slot.shape, mig_slot.dtype),
            pltpu.SMEM(table.shape, table.dtype),
            pltpu.VMEM(queries.shape, dtype),
            pltpu.VMEM(keys.shape, dtype),
            pltpu.VMEM(values.shape, dtype),
            pltpu.VMEM(key_pool.shape, dtype),
            pltpu.VMEM(key_pool.shape, dtype),
            pltpu.VMEM(moved, dtype),
            pltpu.VMEM(moved, dtype),
            pltpu.VMEM(guests, dtype),
            pltpu.VMEM(guests, dtype),
            pltpu.VMEM((slots, heads_all, DH), jnp.float32),
            pltpu.VMEM(part, dtype),
            pltpu.VMEM((slots, heads_all, DH), dtype),
            pltpu.VMEM((parts,) + part, dtype),
            pltpu.VMEM((parts, heads_here, DH), dtype),
            pltpu.VMEM((heads_all, DH), dtype),
            pltpu.VMEM((parts, slots + 1, heads_here, DH), jnp.float32),
            pltpu.VMEM((parts, 2, heads_here, DH), jnp.float32),
            pltpu.VMEM((others, slots + 1, heads_here, DH), jnp.float32),
            pltpu.VMEM((others, 2, heads_here, DH), jnp.float32),
            pltpu.VMEM((heads_here, DH), dtype),
            pltpu.VMEM((heads_here, DH), dtype),
            pltpu.VMEM(part, jnp.float32),
            pltpu.VMEM(part, jnp.float32),
            pltpu.SemaphoreType.DMA((6,)),
            pltpu.SemaphoreType.DMA((2, cuts)),
            pltpu.SemaphoreType.DMA((2, 12 if extra else 10)),
            pltpu.SemaphoreType.DMA((2, max(2 * extra, 1))),
            pltpu.SemaphoreType.DMA((2, 1)),
            pltpu.SemaphoreType.DMA((2, others)),
            pltpu.SemaphoreType.DMA((2, others)),
            pltpu.SemaphoreType.DMA((2, others)),
            pltpu.SemaphoreType.DMA((2, others)),
            pltpu.SemaphoreType.DMA((2, 1)),
        ],
        compiler_params=pltpu.CompilerParams(
            collective_id=2 + serial, has_side_effects=True, vmem_limit_bytes=32 << 20
        ),
        cost_estimate=pl.CostEstimate(
            flops=4 * H * slots * pages * rows * width,
            bytes_accessed=4 * math.prod(key_pool.shape),
            transcendentals=0,
        ),
    )(lengths, mig_slot, table, queries, keys, values, key_pool, value_pool)


def settle_kernel(
    live_ref,
    result_ref,
    key_ref,
    value_ref,
    out_ref,
    kout_ref,
    vout_ref,
    blank,
    result_sem,
    page_sems,
):
    pages = key_ref.shape[0]
    live = live_ref[0]
    lanes = ((key_ref, kout_ref), (value_ref, vout_ref))
    result = pltpu.make_async_copy(result_ref, out_ref, result_sem)
    result.start()
    blank[...] = jnp.zeros_like(blank)
    for j in range(pages):
        for n, (origin, target) in enumerate(lanes):
            spot = target.at[j]
            pl.when(j < live)(pltpu.make_async_copy(origin.at[j], spot, page_sems.at[n]).start)
            pl.when(j >= live)(pltpu.make_async_copy(blank, spot, page_sems.at[n]).start)
    for n, (origin, target) in enumerate(lanes):
        pltpu.make_async_copy(origin, target, page_sems.at[n]).wait()
    result.wait()


def settled(live, *arrays):
    rows, width = arrays[1].shape[1:]
    return pl.pallas_call(
        settle_kernel,
        out_shape=[jax.ShapeDtypeStruct(a.shape, a.dtype) for a in arrays],
        in_specs=[pl.BlockSpec(memory_space=pltpu.SMEM)]
        + [pl.BlockSpec(memory_space=pltpu.VMEM)] * 3,
        out_specs=[pl.BlockSpec(memory_space=pltpu.HBM)] * 3,
        scratch_shapes=[
            pltpu.VMEM((rows, width), arrays[1].dtype),
            pltpu.SemaphoreType.DMA,
            pltpu.SemaphoreType.DMA((2,)),
        ],
        compiler_params=pltpu.CompilerParams(vmem_limit_bytes=8 << 20),
    )(live, *arrays)


def choose_kernel(page_len, pages, len_ref, mig_ref, dst_ref, out_ref, live_ref):
    replicas = mig_ref.shape[0]
    slots = len_ref.shape[0] // replicas

    def need(source):
        length = len_ref[source * slots + mig_ref[source]]
        return lax.div(length + (page_len - 1), page_len)

    needs = [need(source) for source in range(replicas)]
    distance = dst_ref[0]
    index, base = jnp.int32(0), 0
    for step, rooms, singles in branch_plans(replicas, pages):
        most = jnp.int32(0)
        for source in paired_sources(replicas, step)[::2] if len(rooms) > 1 else []:
            most = jnp.maximum(most, needs[source] + needs[source + 1])
        longest = jnp.int32(0)
        for source in lone_sources(replicas, step) if len(singles) > 1 else []:
            longest = jnp.maximum(longest, needs[source])
        place = jnp.int32(base)
        for room in rooms[:-1]:
            place = place + jnp.where(most > 2 * room, len(singles), 0)
        for single in singles[:-1]:
            place = place + jnp.where(longest > single, 1, 0)
        index = jnp.where(distance == step, place, index)
        base += len(rooms) * len(singles)
    out_ref[0] = index
    live_ref[0] = need(lax.rem(lax.axis_index("rep") + replicas - distance, replicas))


def chosen(page_len, pages, lengths, mig_slot, mig_dst):
    return pl.pallas_call(
        functools.partial(choose_kernel, page_len, pages),
        out_shape=[pltpu.SMEM((1,), jnp.int32)] * 2,
        in_specs=[pl.BlockSpec(memory_space=pltpu.SMEM)] * 3,
        out_specs=[pl.BlockSpec(memory_space=pltpu.SMEM)] * 2,
    )(lengths, mig_slot, mig_dst)


def swift_body(
    queries, new_keys, new_values, key_pool, value_pool, lengths, page_table, mig_slot, mig_dst
):
    replicas = lax.axis_size("rep")
    pages = page_table.shape[1]
    page_len = key_pool.shape[1] * lax.axis_size("tp")
    plans = [
        (distance, room, single)
        for distance, rooms, singles in branch_plans(replicas, pages)
        for room in rooms
        for single in singles
    ]
    index, live = chosen(page_len, pages, lengths, mig_slot, mig_dst)
    results = lax.switch(
        index[0],
        [functools.partial(served, n, *plan) for n, plan in enumerate(plans)],
        lengths,
        mig_slot,
        page_table,
        queries,
        new_keys,
        new_values,
        key_pool,
        value_pool,
    )
    return settled(live, *results)


def solution(mesh):
    placed = (
        P("rep", "tp"),
        P("rep", "tp"),
        P("rep", "tp"),
        P("rep", "tp", None),
        P("rep", "tp", None),
        P(),
        P("rep", None),
        P(),
        P(),
    )
    swift = KVH % mesh.shape["tp"] == 0
    return jax.shard_map(
        swift_body if swift else body,
        mesh=mesh,
        in_specs=placed,
        out_specs=(P("rep", "tp"), P("rep", "tp", None), P("rep", "tp", None)),
        check_vma=False,
    )
```
